256 devices in a mesh: groups: 2 (over z), section: 2 (over core), mesh: 64 (over x, y).
Axes of the slice: x: 8, y: 8, z: 2, core: 2. Of those that a mesh axis runs over, the one named last changes fastest.
The devices are a block of a 8x8x16 slice.
Arguments:
- inputs: bfloat16 [4, 128, 8192], P('groups', None, 'mesh'), parts along dimension 0, may hold values from -12 to 12
- segments: int32 [4, 128], P('groups'), parts along dimension 0, may hold values from 0 to 3, never falling along the last dimension, each value on 1 to 64 neighbouring positions
- gains: bfloat16 [2, 1, 8192], P('section'), may hold values from 0.25 to 1.75
- w_query: bfloat16 [2, 1, 8192, 8192], P('section', None, None, 'mesh'), may hold values from -1.3258252 to 1.3258252
- w_keyval: bfloat16 [2, 1, 8192, 2048], P('section', None, None, 'mesh'), may hold values from -0.055242717 to 0.055242717
- w_output: bfloat16 [2, 1, 8192, 8192], P('section', None, None, 'mesh'), may hold values from -0.0625 to 0.0625
Outputs:
- section_outputs: bfloat16 [2, 4, 128, 8192], P('section', 'groups', None, 'mesh'), parts along dimension 1
The draws below stay inside these ranges and needn't reach their ends.
There are 2 independent parts, one for each index of `groups`. The reference program is written for one: setup_inputs(seed, part) draws one part's arguments, and reference() takes and returns one part's arrays. A program takes and returns all parts, laid end to end along the dimension named above; an argument that names none is the same for every part. Nothing has to cross between parts.
Inputs may be any that keep to these rules, and one draw needn't show every extreme that they name: `segments`: along each micro-batch the document ids never fall; each document spans 1 to 64 positions.
All inputs are finite; a program needn't handle non-finite values.
Results may differ from the reference program's by a relative error of at most 0.0052.
Values may be sent and summed in bfloat16 or wider, within the bound.
No kernel may reach another device: no remote copies, remote signals or barrier semaphores. Data moves between devices by JAX's collectives and lax.ppermute only.
A program may use at most 64 MiB of HBM per device.

```python
import math
import jax
import jax.numpy as jnp
import numpy as np
from jax import lax

D = 8192
HD = 128
GROUP = 8
TOK = 128
MICRO = 2
LAYERS = 1
HEADS = 64
KVH = 8
SECTIONS = 2
SEGS = 4


def keyval_base(key):
    shape_kv = (SECTIONS, LAYERS, D, KVH * 2 * HD)
    base = jax.random.normal(jax.random.fold_in(key, 11), shape_kv, jnp.float32)
    return jnp.clip(base, -5.0, 5.0) / math.sqrt(D)


def draw_w_keyval(key, part):
    return keyval_base(key).astype(jnp.bfloat16)


def draw_w_query(key, part):
    value = jnp.clip(jax.random.normal(jax.random.fold_in(key, 19), (SECTIONS, LAYERS, D, HEADS, HD), jnp.float32), -5.0, 5.0) / math.sqrt(D)
    return value.reshape(SECTIONS, LAYERS, D, HEADS * HD).astype(jnp.bfloat16)


def draw_inputs(key, part):
    columns = jnp.arange(D, dtype=jnp.int32).astype(jnp.float32)
    rising = jnp.sqrt(1.0 + 2.0 * columns / D)
    rough = jnp.exp(jax.random.uniform(jax.random.fold_in(key, 3), (D,), jnp.float32, math.log(0.7), math.log(1.4)))
    base = jax.random.normal(jax.random.fold_in(key, 5), (MICRO, TOK, D), jnp.float32)
    value = base
    return jnp.clip(value * rising * rough, -12.0, 12.0).astype(jnp.bfloat16)


def levels(own_key, dims, shards, smallest, high):
    def one(dim, parts):
        steps = jax.random.uniform(jax.random.fold_in(jax.random.fold_in(own_key, 6), dim), (parts,), jnp.float32, smallest / len(shards), high / len(shards))
        return jnp.repeat(jnp.exp(steps), dims[dim] // parts).reshape((-1,) + (1,) * (len(dims) - dim - 1))

    loudness = one(*shards[0])
    for cut in shards[1:]:
        loudness = loudness * one(*cut)
    return loudness


def profile(number_of, total, limit, lean):
    loads = [(1 << 20) // math.isqrt(rank ** lean) + 1 for rank in range(2, number_of + 1)]
    rest, given = total - limit - (number_of - 1), [1] * (number_of - 1)
    while rest > 0:
        movable = [i for i in range(number_of - 1) if given[i] < limit]
        mass, left = sum([loads[i] for i in movable]), rest
        for i in movable:
            extra = min(limit - given[i], max(1, left * loads[i] // mass), rest)
            given[i] = given[i] + extra
            rest = rest - extra
    return np.array([limit] + given)


def uneven_parts(rng, number_of, total, reach, slope):
    if number_of == 2:
        one = jax.random.randint(rng, (), max(1, total - reach), min(reach, total - 1) + 1)
        return jnp.stack([one, total - one])
    lengths = jnp.asarray(profile(number_of, total, reach, slope), jnp.int32)
    pairs = (number_of - 1) // 2
    donor, taker = lengths[1:1 + 2 * pairs:2], lengths[2:2 + 2 * pairs:2]
    slack = jnp.minimum(donor - 1, reach - taker)
    moved = jax.random.randint(jax.random.fold_in(rng, 1), (pairs,), 0, 1 << 20) % (slack + 1)
    lengths = lengths.at[1:1 + 2 * pairs:2].set(donor - moved).at[2:2 + 2 * pairs:2].set(taker + moved)
    return lengths[jax.random.permutation(jax.random.fold_in(rng, 2), number_of)]


def bell_draw(stream_key, shape, scale, limit, shards=(), kind=jnp.bfloat16):
    drawn = jax.random.normal(stream_key, shape, jnp.float32) * scale
    if len(shards) > 0:
        drawn = levels(stream_key, shape, shards, -0.22, 0.18) * drawn
    return jnp.clip(drawn, min=-limit, max=limit).astype(kind)


def setup_inputs(seed: int = 0, part: int = 0) -> dict:
    seeds = jax.random.split(jax.random.key(seed), 7)
    own_keys = jax.random.split(jax.random.fold_in(seeds[6], part), 7)
    return {
        "inputs": draw_inputs(jax.random.fold_in(jax.random.fold_in(seeds[6], part), 71), part),
        "segments": jax.vmap(lambda own: jnp.searchsorted(jnp.cumsum(uneven_parts(own, SEGS, TOK, TOK // 2, 1)), jnp.arange(TOK), side="right"))(jax.random.split(own_keys[1], MICRO)).reshape((MICRO, TOK)).astype(jnp.int32),
        "gains": jnp.clip(1.0 + 0.15 * jax.random.normal(seeds[2], (SECTIONS, LAYERS, D), jnp.float32), 0.25, 1.75).astype(jnp.bfloat16),
        "w_query": draw_w_query(jax.random.fold_in(seeds[6], 71), part),
        "w_keyval": draw_w_keyval(jax.random.fold_in(seeds[6], 71), part),
        "w_output": bell_draw(seeds[5], (SECTIONS, LAYERS, HEADS * HD, D), (HEADS * HD) ** -0.5, 0.0625, ((0, 2), (3, 64))),
    }


norm_epsilon = 1e-05
rope_theta = 500000.0

def position_tables(segment_row):
    row_length = segment_row.shape[0]
    indices = jnp.arange(row_length, dtype=jnp.int32)
    doc_starts = jnp.concatenate([jnp.ones((1,), dtype=bool), segment_row[1:] != segment_row[:-1]])
    first_index = lax.cummax(jnp.where(doc_starts, indices, jnp.zeros_like(indices)), axis=0)
    positions = (indices - first_index).astype(jnp.float32)
    half_width = HD // 2
    freqs = rope_theta ** (-(2.0 * jnp.arange(half_width, dtype=jnp.float32)) / HD)
    angles = positions[:, None] * freqs[None, :]
    cosine_table = jnp.concatenate([jnp.cos(angles), jnp.cos(angles)], axis=1)
    sine_table = jnp.concatenate([jnp.sin(angles), jnp.sin(angles)], axis=1)
    allowed = (indices[None, :] <= indices[:, None]) & (segment_row[None, :] == segment_row[:, None])
    return (cosine_table, sine_table, allowed)

def rotate(values, cosine_table, sine_table):
    half_width = values.shape[-1] // 2
    turned = jnp.concatenate([-values[..., half_width:], values[..., :half_width]], axis=-1)
    return values * cosine_table + turned * sine_table

def softmax_weights(scores, allowed):
    masked = jnp.where(allowed, scores, -1e+30)
    highest = lax.optimization_barrier(jnp.max(masked, axis=-1, keepdims=True))
    raised = jnp.exp(masked - highest)
    return (raised / lax.optimization_barrier(jnp.sum(raised, axis=-1, keepdims=True))).astype(jnp.bfloat16)

def apply_layer(activations, gain_row, query_weight, keyval_weight, output_weight, tables):
    cosine_table, sine_table, allowed = tables
    floats = activations.astype(jnp.float32)
    row_count = floats.shape[0]
    scale = lax.rsqrt(lax.optimization_barrier(jnp.mean(floats * floats, axis=1, keepdims=True)) + norm_epsilon)
    normed = (floats * scale * gain_row.astype(jnp.float32)).astype(jnp.bfloat16)
    query = jnp.dot(normed, query_weight, preferred_element_type=jnp.float32).reshape(row_count, HEADS, HD)
    query = rotate(query, cosine_table[:, None, :], sine_table[:, None, :]).astype(jnp.bfloat16)
    keyval = jnp.dot(normed, keyval_weight, preferred_element_type=jnp.float32).astype(jnp.bfloat16)
    keyval = keyval.reshape(row_count, KVH, 2, HD)
    keys = rotate(keyval[:, :, 0, :].astype(jnp.float32), cosine_table[:, None, :], sine_table[:, None, :]).astype(jnp.bfloat16)
    values = keyval[:, :, 1, :]
    grouped = query.reshape(row_count, KVH, GROUP, HD)
    scores = jnp.einsum('tgqd,sgd->gqts', grouped.astype(jnp.float32), keys.astype(jnp.float32)) * HD ** (-0.5)
    probs = softmax_weights(scores, allowed[None, None, :, :])
    attended = jnp.einsum('gqts,sgd->tgqd', probs.astype(jnp.float32), values.astype(jnp.float32))
    attended = attended.astype(jnp.bfloat16).reshape(row_count, HEADS * HD)
    mixed = jnp.dot(attended, output_weight, preferred_element_type=jnp.float32)
    return (floats + mixed).astype(jnp.bfloat16)

def reference(inputs, segments, gains, w_query, w_keyval, w_output):
    tables = [position_tables(segments[micro_index]) for micro_index in range(MICRO)]
    current = [inputs[micro_index] for micro_index in range(MICRO)]
    results = []
    for section_index in range(SECTIONS):
        for micro_index in range(MICRO):
            for layer_index in range(LAYERS):
                current[micro_index] = apply_layer(current[micro_index], gains[section_index, layer_index], w_query[section_index, layer_index], w_keyval[section_index, layer_index], w_output[section_index, layer_index], tables[micro_index])
        results.append(jnp.stack(current))
    return jnp.stack(results)
```

```python
import functools

import jax
import jax.numpy as jnp
from jax import lax
from jax.experimental import pallas as pl
from jax.experimental.pallas import tpu as pltpu
from jax.sharding import Mesh
from jax.sharding import PartitionSpec as P

HD = 128
HALF = HD // 2
X = ("x2", "x1", "x0")
Y = ("y2", "y1", "y0")
MESH = X + Y
norm_epsilon = 1e-05
rope_theta = 500000.0
VMEM_LIMIT = 56 * 1024 * 1024


def position_tables(segment_row):
    row_length = segment_row.shape[0]
    indices = jnp.arange(row_length, dtype=jnp.int32)
    same = segment_row[None, :] == segment_row[:, None]
    first_index = jnp.min(jnp.where(same, indices[None, :], row_length), axis=1)
    positions = (indices - first_index).astype(jnp.float32)
    freqs = rope_theta ** (-(2.0 * jnp.arange(HALF, dtype=jnp.float32)) / HD)
    angles = positions[:, None] * freqs[None, :]
    cosine, sine = jnp.cos(angles), jnp.sin(angles)
    allowed = (indices[None, :] <= indices[:, None]) & same
    return (
        jnp.concatenate([cosine, cosine], axis=1),
        jnp.concatenate([-sine, sine], axis=1),
        allowed.astype(jnp.float32),
    )


def project_kernel(pick, blocks, gain, wq_a, wq_b, wkv_a, wkv_b, cosine, sine, query, keyval):
    count, rows, width = blocks.shape
    second = pick[0] == 1
    total = jnp.zeros((rows, width), jnp.float32)
    for d in range(count):
        part = blocks[d].astype(jnp.float32)
        total += part * part
    scale = lax.rsqrt(
        jnp.sum(total, axis=1, keepdims=True) / (count * width) + norm_epsilon
    )
    q_sum = jnp.zeros(query.shape, jnp.float32)
    kv_sum = jnp.zeros((rows, wkv_a.shape[1]), jnp.float32)
    for d in range(0, count, 2):
        pair = []
        for e in (d, d + 1):
            weight = gain[:, e * width : (e + 1) * width].astype(jnp.float32)
            pair.append((blocks[e].astype(jnp.float32) * scale * weight).astype(jnp.bfloat16))
        normed = jnp.concatenate(pair, axis=1)
        span = slice(d * width, (d + 2) * width)
        wq = jnp.where(second, wq_b[span, :], wq_a[span, :])
        wkv = jnp.where(second, wkv_b[span, :], wkv_a[span, :])
        q_sum += jnp.dot(normed, wq, preferred_element_type=jnp.float32)
        kv_sum += jnp.dot(normed, wkv, preferred_element_type=jnp.float32)
    turned = jnp.concatenate([q_sum[:, HALF:], q_sum[:, :HALF]], axis=1)
    query[...] = (q_sum * cosine[...] + turned * sine[...]).astype(query.dtype)
    flat = kv_sum.astype(jnp.bfloat16).astype(jnp.float32).T.astype(jnp.bfloat16)
    keyval[...] = jnp.broadcast_to(flat[None], keyval.shape)


def attend_kernel(query, keyval, cosine, sine, allowed, attended):
    keys = keyval[:HD, :].astype(jnp.float32)
    turned = jnp.concatenate([keys[HALF:], keys[:HALF]], axis=0)
    keys = (keys * cosine[...].T + turned * sine[...].T).astype(jnp.bfloat16)
    scores = jnp.dot(query[...], keys, preferred_element_type=jnp.float32) * HD ** (-0.5)
    masked = jnp.where(allowed[...] > 0.0, scores, -1e30)
    highest = jnp.max(masked, axis=1, keepdims=True)
    raised = jnp.exp(masked - highest)
    probs = (raised / jnp.sum(raised, axis=1, keepdims=True)).astype(jnp.bfloat16)
    out = lax.dot_general(
        probs, keyval[HD:, :], (((1,), (1,)), ((), ())), preferred_element_type=jnp.float32
    ).astype(jnp.bfloat16)
    attended[...] = jnp.broadcast_to(out[None], attended.shape)


def mix_kernel(pick, blocks, wo_a, wo_b, residual, result, copies=None):
    count, rows, width = blocks.shape
    second = pick[0] == 1
    mixed = residual[...].astype(jnp.float32)
    for d in range(0, count, 2):
        pair = jnp.concatenate([blocks[d], blocks[d + 1]], axis=1)
        span = slice(d * width, (d + 2) * width)
        wo = jnp.where(second, wo_b[span, :], wo_a[span, :])
        mixed += jnp.dot(pair, wo, preferred_element_type=jnp.float32)
    out = mixed.astype(result.dtype)
    result[...] = out
    if copies is not None:
        copies[...] = jnp.broadcast_to(out[None], copies.shape)


def call(kernel, outs, n_in, scalar_first):
    vmem = pl.BlockSpec(memory_space=pltpu.VMEM)
    specs = [pl.BlockSpec(memory_space=pltpu.SMEM)] if scalar_first else []
    specs += [vmem] * (n_in - len(specs))
    return pl.pallas_call(
        kernel,
        out_shape=outs,
        in_specs=specs,
        out_specs=jax.tree.map(lambda _: vmem, outs),
        compiler_params=pltpu.CompilerParams(vmem_limit_bytes=VMEM_LIMIT),
    )


def exchange(copies):
    return lax.all_to_all(copies, MESH, 0, 0, tiled=True)


def shards(inputs, segments, gains, w_query, w_keyval, w_output):
    _, rows, width = inputs.shape
    sections = lax.axis_size("section")
    devices = lax.axis_size(MESH)
    ring = lax.axis_size(Y)
    me = lax.axis_index("section")
    swap = [(0, 1), (1, 0)]
    own = [w[0, 0] for w in (w_query, w_keyval, w_output)]
    current = lax.dynamic_index_in_dim(inputs, me, 0, keepdims=False)
    segment_row = lax.dynamic_index_in_dim(segments, me, 0, keepdims=False)
    cosine, sine, allowed = position_tables(segment_row)
    other_gain = lax.ppermute(gains[0], "section", swap)
    other = [lax.ppermute(w, "section", swap) for w in own]
    copies = jnp.broadcast_to(current[None], (devices, rows, width))
    bf16 = functools.partial(jax.ShapeDtypeStruct, dtype=jnp.bfloat16)
    results = []
    for s in range(sections):
        pick = jnp.where(me == s, 0, 1).astype(jnp.int32).reshape(1)
        gain = jnp.where(me == s, gains[0], other_gain)
        blocks = exchange(copies)
        query, keyval = call(
            project_kernel, (bf16((rows, width)), bf16((ring, own[1].shape[1], rows))), 9, True
        )(pick, blocks, gain, own[0], other[0], own[1], other[1], cosine, sine)
        keyval = lax.all_to_all(keyval, Y, 0, 0, tiled=True).reshape(-1, rows)
        attended = call(attend_kernel, bf16((devices, rows, width)), 5, False)(
            query, keyval, cosine, sine, allowed
        )
        blocks = exchange(attended)
        outs = (bf16((rows, width)),)
        if s + 1 < sections:
            outs += (bf16((devices, rows, width)),)
        current, *copies = call(mix_kernel, outs, 5, True)(pick, blocks, own[2], other[2], current)
        copies = copies[0] if copies else None
        results.append(current)
    mine = jnp.where(me == 0, results[0], results[1])
    theirs = lax.ppermute(jnp.where(me == 0, results[1], results[0]), "section", swap)
    first = jnp.where(me == 0, mine, theirs)
    second = jnp.where(me == 0, theirs, mine)
    return jnp.stack([first, second])[None]


def solution(mesh):
    finer = Mesh(
        mesh.devices.reshape(mesh.shape["groups"], mesh.shape["section"], *([2] * 6)),
        ("groups", "section") + MESH,
    )
    in_specs = (
        P("groups", None, MESH),
        P("groups", None),
        P("section", None, None),
        P("section", None, None, MESH),
        P("section", None, None, MESH),
        P("section", None, None, MESH),
    )
    out_specs = P("section", "groups", None, MESH)
    return jax.shard_map(
        shards, mesh=finer, in_specs=in_specs, out_specs=out_specs, check_vma=False
    )
```

```python
import functools

import jax
import jax.numpy as jnp
from jax import lax
from jax.experimental import pallas as pl
from jax.experimental.pallas import tpu as pltpu
from jax.sharding import Mesh
from jax.sharding import PartitionSpec as P

HD = 128
HALF = HD // 2
X = ("x2", "x1", "x0")
Y = ("y2", "y1", "y0")
MESH = X + Y
FAR = ("x2", "x1", "y2", "y1")
SIDE = 8
FAR_COUNT = 16
PLACES = [SIDE * 2 * (j // 4) + 2 * (j % 4) for j in range(FAR_COUNT)]
norm_epsilon = 1e-05
rope_theta = 500000.0
MIB = 1024 * 1024


def position_tables(segment_row):
    row_length = segment_row.shape[0]
    indices = jnp.arange(row_length, dtype=jnp.int32)
    same = segment_row[None, :] == segment_row[:, None]
    first_index = jnp.min(jnp.where(same, indices[None, :], row_length), axis=1)
    positions = (indices - first_index).astype(jnp.float32)
    freqs = rope_theta ** (-(2.0 * jnp.arange(HALF, dtype=jnp.float32)) / HD)
    angles = positions[:, None] * freqs[None, :]
    cosine, sine = jnp.cos(angles), jnp.sin(angles)
    allowed = (indices[None, :] <= indices[:, None]) & same
    return (
        jnp.concatenate([cosine, cosine], axis=1),
        jnp.concatenate([-sine, sine], axis=1),
        allowed.astype(jnp.float32),
    )


LAYOUT = ((0, 0), (1, 0), (1, 8), (2, 0), (2, 8), (3, 0), (3, 4), (3, 8), (3, 12))


def all_blocks(bases, buffers, layout):
    for ref, (kind, first) in zip(buffers, layout, strict=True):
        for j in range(ref.shape[0]):
            yield ref, j, bases[kind] + PLACES[first + j]


def rows_at(place, width):
    return pl.ds(pl.multiple_of(place * width, width), width)


def weight_pair(second, own, other, places, width):
    halves = []
    for place in places:
        span = rows_at(place, width)
        halves.append(jnp.where(second, other[span, :], own[span, :]))
    return jnp.concatenate(halves, axis=0)


def pairs_of(blocks):
    blocks = list(blocks)
    return zip(blocks[0::2], blocks[1::2], strict=True)


def normed_pair(pair, scale, gain):
    parts = []
    for ref, j, place in pair:
        scaled = ref[j].astype(jnp.float32) * scale * gain[place]
        parts.append(scaled.astype(jnp.bfloat16))
    return jnp.concatenate(parts, axis=1)


def keyval_kernel(info, gain, own, other, *rest):
    buffers, (scale_out, keyval) = rest[: len(LAYOUT)], rest[len(LAYOUT) :]
    second, bases = info[0] == 1, [info[1 + k] for k in range(4)]
    rows, width = scale_out.shape
    total = jnp.zeros((rows, width), jnp.float32)
    blocks = list(all_blocks(bases, buffers, LAYOUT))
    for ref, j, _ in blocks:
        part = ref[j].astype(jnp.float32)
        total += part * part
    mean = jnp.sum(total, axis=1, keepdims=True) / (len(blocks) * width)
    scale = lax.rsqrt(mean + norm_epsilon)
    scale_out[...] = jnp.broadcast_to(scale, (rows, width))
    kv_sum = jnp.zeros((rows, own.shape[1]), jnp.float32)
    for pair in pairs_of(blocks):
        weight = weight_pair(second, own, other, [p[2] for p in pair], width)
        kv_sum += jnp.dot(
            normed_pair(pair, scale, gain), weight, preferred_element_type=jnp.float32
        )
    flat = kv_sum.T.astype(jnp.bfloat16)
    keyval[...] = jnp.broadcast_to(flat[None], keyval.shape)


def query_kernel(info, gain, own, other, scale_in, cosine, sine, *rest):
    buffers, (query,) = rest[: len(LAYOUT)], rest[len(LAYOUT) :]
    second, bases = info[0] == 1, [info[1 + k] for k in range(4)]
    rows, width = scale_in.shape
    scale = scale_in[...]
    q_sum = jnp.zeros((rows, width), jnp.float32)
    for pair in pairs_of(all_blocks(bases, buffers, LAYOUT)):
        weight = weight_pair(second, own, other, [p[2] for p in pair], width)
        q_sum += jnp.dot(
            normed_pair(pair, scale, gain), weight, preferred_element_type=jnp.float32
        )
    turned = jnp.concatenate([q_sum[:, HALF:], q_sum[:, :HALF]], axis=1)
    query[...] = (q_sum * cosine[...] + turned * sine[...]).astype(query.dtype)


def attend_kernel(query, keyval, cosine, sine, allowed, attended):
    keys = keyval[:HD, :].astype(jnp.float32)
    turned = jnp.concatenate([keys[HALF:], keys[:HALF]], axis=0)
    keys = (keys * cosine[...].T + turned * sine[...].T).astype(jnp.bfloat16)
    scores = jnp.dot(query[...], keys, preferred_element_type=jnp.float32) * HD ** (-0.5)
    masked = jnp.where(allowed[...] > 0.0, scores, -1e30)
    highest = jnp.max(masked, axis=1, keepdims=True)
    raised = jnp.exp(masked - highest)
    probs = (raised / jnp.sum(raised, axis=1, keepdims=True)).astype(jnp.bfloat16)
    out = lax.dot_general(
        probs, keyval[HD:, :], (((1,), (1,)), ((), ())), preferred_element_type=jnp.float32
    ).astype(jnp.bfloat16)
    attended[...] = jnp.broadcast_to(out[None], attended.shape)


def mix_kernel(layout, info, own, other, before, *rest):
    buffers, outs = rest[: len(layout)], rest[len(layout) :]
    second, bases = info[0] == 1, [info[1 + k] for k in range(4)]
    width = before.shape[1]
    mixed = before[...].astype(jnp.float32)
    for pair in pairs_of(all_blocks(bases, buffers, layout)):
        weight = weight_pair(second, own, other, [p[2] for p in pair], width)
        both = jnp.concatenate([ref[j] for ref, j, _ in pair], axis=1)
        mixed += jnp.dot(both, weight, preferred_element_type=jnp.float32)
    out = mixed.astype(outs[0].dtype)
    outs[0][...] = out
    if len(outs) > 1:
        outs[1][...] = jnp.broadcast_to(out[None], outs[1].shape)


def call(kernel, outs, limit, *args, scalars=True):
    vmem = pl.BlockSpec(memory_space=pltpu.VMEM)
    specs = [vmem] * len(args)
    if scalars:
        specs[0] = pl.BlockSpec(memory_space=pltpu.SMEM)
    return pl.pallas_call(
        kernel,
        out_shape=outs,
        in_specs=specs,
        out_specs=jax.tree.map(lambda _: vmem, outs),
        compiler_params=pltpu.CompilerParams(vmem_limit_bytes=limit * MIB),
    )(*args)


def from_neighbour(block, dx, dy):
    pairs = []
    for x in range(SIDE):
        for y in range(SIDE):
            there = (x + dx) % SIDE * SIDE + (y + dy) % SIDE
            pairs.append((there, x * SIDE + y))
    return lax.ppermute(block, MESH, pairs)


def far_stage(copies):
    return lax.all_to_all(copies, FAR, 0, 0, tiled=True)


def near_stage(own):
    low, high = own[:8], own[8:]
    xa, xb = from_neighbour(low, 1, 0), from_neighbour(high, -1, 0)
    ya, yb = from_neighbour(low, 0, 1), from_neighbour(high, 0, -1)
    quarters = (
        from_neighbour(ya[:4], 1, 0),
        from_neighbour(ya[4:], -1, 0),
        from_neighbour(xb[:4], 0, 1),
        from_neighbour(xb[4:], 0, -1),
    )
    return (own,), (xa, xb, ya, yb), quarters


def shards(inputs, segments, gains, w_query, w_keyval, w_output):
    _, rows, width = inputs.shape
    sections = lax.axis_size("section")
    ring = lax.axis_size(Y)
    devices = lax.axis_size(MESH)
    me = lax.axis_index("section")
    px, py = lax.axis_index("x0"), lax.axis_index("y0")
    swap = [(0, 1), (1, 0)]
    own = [w[0, 0] for w in (w_query, w_keyval, w_output)]
    current = lax.dynamic_index_in_dim(inputs, me, 0, keepdims=False)
    segment_row = lax.dynamic_index_in_dim(segments, me, 0, keepdims=False)
    cosine, sine, allowed = position_tables(segment_row)
    other_gain = lax.ppermute(gains[0], "section", swap)
    other = [lax.ppermute(w, "section", swap) for w in own]
    copies = jnp.broadcast_to(current[None], (FAR_COUNT, rows, width))
    shape = jax.ShapeDtypeStruct
    bf16 = functools.partial(shape, dtype=jnp.bfloat16)
    f32 = functools.partial(shape, dtype=jnp.float32)
    bases = jnp.stack(
        [
            SIDE * px + py,
            SIDE * (1 - px) + py,
            SIDE * px + (1 - py),
            SIDE * (1 - px) + (1 - py),
        ]
    )
    results = []
    for s in range(sections):
        pick = jnp.where(me == s, 0, 1)
        info = jnp.concatenate([pick[None], bases]).astype(jnp.int32)
        gain = jnp.where(me == s, gains[0], other_gain)
        gain = gain.astype(jnp.float32).reshape(devices, 1, width)
        near = near_stage(far_stage(copies))
        blocks = [b for group in near for b in group]
        scale, keyval = call(
            keyval_kernel,
            (f32((rows, width)), bf16((ring, own[1].shape[1], rows))),
            16,
            info,
            gain,
            own[1],
            other[1],
            *blocks,
        )
        keyval = lax.all_to_all(keyval, Y, 0, 0, tiled=True).reshape(-1, rows)
        query = call(
            query_kernel,
            bf16((rows, width)),
            16,
            info,
            gain,
            own[0],
            other[0],
            scale,
            cosine,
            sine,
            *blocks,
        )
        attended = call(
            attend_kernel,
            bf16((FAR_COUNT, rows, width)),
            8,
            query,
            keyval,
            cosine,
            sine,
            allowed,
            scalars=False,
        )
        near = near_stage(far_stage(attended))
        layouts = (LAYOUT[:1], LAYOUT[1:5], LAYOUT[5:])
        partial = current
        for k, (group, layout) in enumerate(zip(near, layouts, strict=True)):
            outs = (f32((rows, width)),)
            if k == len(layouts) - 1:
                outs = (bf16((rows, width)),)
                if s + 1 < sections:
                    outs += (bf16((FAR_COUNT, rows, width)),)
            kernel = functools.partial(mix_kernel, layout)
            partial, *copies = call(kernel, outs, 12, info, own[2], other[2], partial, *group)
        copies = copies[0] if copies else None
        current = partial
        results.append(current)
    mine = jnp.where(me == 0, results[0], results[1])
    theirs = lax.ppermute(jnp.where(me == 0, results[1], results[0]), "section", swap)
    first = jnp.where(me == 0, mine, theirs)
    second = jnp.where(me == 0, theirs, mine)
    return jnp.stack([first, second])[None]


def solution(mesh):
    finer = Mesh(
        mesh.devices.reshape(mesh.shape["groups"], mesh.shape["section"], *([2] * 6)),
        ("groups", "section") + MESH,
    )
    in_specs = (
        P("groups", None, MESH),
        P("groups", None),
        P("section", None, None),
        P("section", None, None, MESH),
        P("section", None, None, MESH),
        P("section", None, None, MESH),
    )
    out_specs = P("section", "groups", None, MESH)
    return jax.shard_map(
        shards, mesh=finer, in_specs=in_specs, out_specs=out_specs, check_vma=False
    )
```

```python
import functools

import jax
import jax.numpy as jnp
from jax import lax
from jax.experimental import pallas as pl
from jax.experimental.pallas import tpu as pltpu
from jax.sharding import Mesh
from jax.sharding import PartitionSpec as P

HD = 128
HALF = HD // 2
X = ("x2", "x1", "x0")
Y = ("y2", "y1", "y0")
MESH = X + Y
FAR = ("x2", "x1", "y2", "y1")
SIDE = 8
FAR_COUNT = 16
norm_epsilon = 1e-05
rope_theta = 500000.0
MIB = 1024 * 1024


def position_tables(segment_row):
    row_length = segment_row.shape[0]
    indices = jnp.arange(row_length, dtype=jnp.int32)
    same = segment_row[None, :] == segment_row[:, None]
    first_index = jnp.min(jnp.where(same, indices[None, :], row_length), axis=1)
    positions = (indices - first_index).astype(jnp.float32)
    freqs = rope_theta ** (-(2.0 * jnp.arange(HALF, dtype=jnp.float32)) / HD)
    angles = positions[:, None] * freqs[None, :]
    cosine, sine = jnp.cos(angles), jnp.sin(angles)
    allowed = (indices[None, :] <= indices[:, None]) & same
    return (
        jnp.concatenate([cosine, cosine], axis=1),
        jnp.concatenate([-sine, sine], axis=1),
        allowed.astype(jnp.float32),
    )


STAGES = (
    ((0, 0, 0),),
    ((1, 0, 0), (1, 0, 8), (0, 1, 0), (0, 1, 8)),
    ((1, 1, 0), (1, 1, 8)),
)
STEP = 4


def for_chunks(buffers, layout, body, carry):
    px, py = lax.axis_index("x0"), lax.axis_index("y0")
    for ref, (turn_x, turn_y, first) in zip(buffers, layout, strict=True):
        base = SIDE * jnp.where(turn_x == 1, 1 - px, px) + jnp.where(turn_y == 1, 1 - py, py)
        base += 2 * SIDE * (first // STEP)

        def chunk(i, carry, ref=ref, base=base):
            place = base + 2 * SIDE * i
            return body([(ref[i * STEP + k], place + 2 * k) for k in range(STEP)], carry)

        count = ref.shape[0] // STEP
        carry = chunk(0, carry) if count == 1 else lax.fori_loop(0, count, chunk, carry)
    return carry


def at(place, width):
    return pl.ds(pl.multiple_of(place * width, width), width)


def is_other(section):
    return lax.axis_index("section") != section


def weight_rows(second, own, other, chunk, width):
    parts = []
    for _, place in chunk:
        parts.append(jnp.where(second, other[at(place, width), :], own[at(place, width), :]))
    return jnp.concatenate(parts, axis=0)


def project_kernel(
    section, layout, first, last, gain_own, gain_other, own, other, kv_own, kv_other, *rest
):
    before = () if first else rest[:3]
    rest = rest[len(before) :]
    tables = rest[:2] if last else ()
    rest = rest[len(tables) :]
    buffers, outs = rest[: len(layout)], rest[len(layout) :]
    second = is_other(section)
    rows, width = buffers[0].shape[1:]
    columns = kv_own.shape[0]

    def body(chunk, carry):
        q_sum, kv_sum, squares = carry
        scaled, kv_parts = [], []
        for part, place in chunk:
            gain = jnp.where(second, gain_other[place], gain_own[place])
            wide = part.astype(jnp.float32)
            squares += wide * wide
            scaled.append((wide * gain).astype(jnp.bfloat16))
            span = at(place, width)
            kv_parts.append(jnp.where(second, kv_other[:, span], kv_own[:, span]))
        scaled = jnp.concatenate(scaled, axis=1)
        weight = weight_rows(second, own, other, chunk, width)
        q_sum += jnp.dot(scaled, weight, preferred_element_type=jnp.float32)
        kv_sum += lax.dot_general(
            jnp.concatenate(kv_parts, axis=1),
            scaled,
            (((1,), (1,)), ((), ())),
            preferred_element_type=jnp.float32,
        )
        return q_sum, kv_sum, squares

    if first:
        carry = tuple(
            jnp.zeros(shape, jnp.float32) for shape in ((rows, width), (columns, rows), (rows, width))
        )
    else:
        carry = tuple(ref[...] for ref in before)
    carry = for_chunks(buffers, layout, body, carry)
    if not last:
        for out, value in zip(outs, carry, strict=True):
            out[...] = value
        return
    q_sum, kv_sum, squares = carry
    cosine, sine = tables
    query, keyval = outs
    features = width * gain_own.shape[0]
    scale = lax.rsqrt(jnp.sum(squares, axis=1, keepdims=True) / features + norm_epsilon)
    q_sum *= scale
    turned = jnp.concatenate([q_sum[:, HALF:], q_sum[:, :HALF]], axis=1)
    query[...] = (q_sum * cosine[...] + turned * sine[...]).astype(query.dtype)
    across = jnp.broadcast_to(scale, (rows, width)).T[:columns, :]
    flat = (kv_sum * across).astype(keyval.dtype)
    keyval[...] = jnp.broadcast_to(flat[None], keyval.shape)


def attend_kernel(query, keyval, cosine, sine, allowed, attended):
    keys = keyval[:HD, :].astype(jnp.float32)
    turned = jnp.concatenate([keys[HALF:], keys[:HALF]], axis=0)
    keys = (keys * cosine[...].T + turned * sine[...].T).astype(jnp.bfloat16)
    scores = jnp.dot(query[...], keys, preferred_element_type=jnp.float32) * HD ** (-0.5)
    masked = jnp.where(allowed[...] > 0.0, scores, -1e30)
    highest = jnp.max(masked, axis=1, keepdims=True)
    raised = jnp.exp(masked - highest)
    probs = (raised / jnp.sum(raised, axis=1, keepdims=True)).astype(jnp.bfloat16)
    out = lax.dot_general(
        probs, keyval[HD:, :], (((1,), (1,)), ((), ())), preferred_element_type=jnp.float32
    ).astype(jnp.bfloat16)
    attended[...] = jnp.broadcast_to(out[None], attended.shape)


def mix_kernel(section, layout, earlier, own, other, before, *rest):
    past, rest = rest[:earlier], rest[earlier:]
    buffers, outs = rest[: len(layout)], rest[len(layout) :]
    second = is_other(section)
    width = before.shape[1]

    def body(chunk, mixed):
        weight = weight_rows(second, own, other, chunk, width)
        joined = jnp.concatenate([part for part, _ in chunk], axis=1)
        return mixed + jnp.dot(joined, weight, preferred_element_type=jnp.float32)

    mixed = for_chunks(buffers, layout, body, before[...].astype(jnp.float32))
    out = mixed.astype(outs[0].dtype)
    if past:
        lower = lax.axis_index("section") == 0
        outs[0][...] = jnp.where(lower, past[0][...], out)
        outs[1][...] = jnp.where(lower, out, past[0][...])
        return
    outs[0][...] = out
    if len(outs) > 1:
        outs[1][...] = jnp.broadcast_to(out[None], outs[1].shape)


def place_kernel(mine, theirs, result):
    me = lax.axis_index("section")
    result[me] = mine[...]
    result[1 - me] = theirs[...]


def call(kernel, outs, limit, *args):
    vmem = pl.BlockSpec(memory_space=pltpu.VMEM)
    return pl.pallas_call(
        kernel,
        out_shape=outs,
        in_specs=[vmem] * len(args),
        out_specs=jax.tree.map(lambda _: vmem, outs),
        compiler_params=pltpu.CompilerParams(vmem_limit_bytes=limit * MIB),
    )(*args)


def from_neighbour(block, dx, dy):
    pairs = []
    for x in range(SIDE):
        for y in range(SIDE):
            there = (x + dx) % SIDE * SIDE + (y + dy) % SIDE
            pairs.append((there, x * SIDE + y))
    return lax.ppermute(block, MESH, pairs)


def far_stage(copies):
    return lax.all_to_all(copies, FAR, 0, 0, tiled=True)


def near_stage(own):
    low, high = own[:8], own[8:]
    xa, xb = from_neighbour(low, 1, 0), from_neighbour(high, -1, 0)
    ya, yb = from_neighbour(low, 0, 1), from_neighbour(high, 0, -1)
    da, db = from_neighbour(xa, 0, 1), from_neighbour(xb, 0, -1)
    return (own,), (xa, xb, ya, yb), (da, db)


def shards(inputs, segments, gains, w_query, w_keyval, w_output):
    _, rows, width = inputs.shape
    sections = lax.axis_size("section")
    ring = lax.axis_size(Y)
    me = lax.axis_index("section")
    swap = [(0, 1), (1, 0)]
    own = [w_query[0, 0], w_keyval[0, 0].T, w_output[0, 0]]
    gain = gains[0].astype(jnp.float32).reshape(-1, 1, width)
    current = lax.dynamic_index_in_dim(inputs, me, 0, keepdims=False)
    segment_row = lax.dynamic_index_in_dim(segments, me, 0, keepdims=False)
    cosine, sine, allowed = position_tables(segment_row)
    copies = jnp.broadcast_to(current[None], (FAR_COUNT, rows, width))
    copies, cosine, sine, allowed, gain = lax.optimization_barrier(
        (copies, cosine, sine, allowed, gain)
    )
    shape = jax.ShapeDtypeStruct
    bf16 = functools.partial(shape, dtype=jnp.bfloat16)
    f32 = functools.partial(shape, dtype=jnp.float32)
    columns = own[1].shape[0]
    stages = len(STAGES)
    for s in range(sections):
        far = far_stage(copies)
        if s == 0:
            far, gain, *own = lax.optimization_barrier((far, gain, *own))
            other_gain = lax.ppermute(gain, "section", swap)
            other = [lax.ppermute(w, "section", swap) for w in own]
        near = near_stage(far)
        sums = ()
        for k, (group, layout) in enumerate(zip(near, STAGES, strict=True)):
            last = k == stages - 1
            outs = (f32((rows, width)), f32((columns, rows)), f32((rows, width)))
            if last:
                outs = (bf16((rows, width)), bf16((ring, columns, rows)))
            kernel = functools.partial(project_kernel, s, layout, k == 0, last)
            tables = (cosine, sine) if last else ()
            weights = (gain, other_gain, own[0], other[0], own[1], other[1])
            sums = call(kernel, outs, 10, *weights, *sums, *tables, *group)
        query, keyval = sums
        keyval = lax.all_to_all(keyval, Y, 0, 0, tiled=True).reshape(-1, rows)
        attended = call(
            attend_kernel, bf16((FAR_COUNT, rows, width)), 4, query, keyval, cosine, sine, allowed
        )
        near = near_stage(far_stage(attended))
        partial, end = current, s + 1 == sections
        for k, (group, layout) in enumerate(zip(near, STAGES, strict=True)):
            outs, past = (f32((rows, width)),), ()
            if k == stages - 1:
                outs = (bf16((rows, width)),)
                past = (current,) if end else ()
                outs += (bf16((rows, width)),) if end else (bf16((FAR_COUNT, rows, width)),)
            kernel = functools.partial(mix_kernel, s, layout, len(past))
            partial, *extra = call(kernel, outs, 10, own[2], other[2], partial, *past, *group)
        current, copies = partial, extra[0]
    theirs = lax.ppermute(copies, "section", swap)
    return call(place_kernel, bf16((sections, rows, width)), 4, current, theirs)[None]


def solution(mesh):
    finer = Mesh(
        mesh.devices.reshape(mesh.shape["groups"], mesh.shape["section"], *([2] * 6)),
        ("groups", "section") + MESH,
    )
    in_specs = (
        P("groups", None, MESH),
        P("groups", None),
        P("section", None, None),
        P("section", None, None, MESH),
        P("section", None, None, MESH),
        P("section", None, None, MESH),
    )
    out_specs = P("section", "groups", None, MESH)
    return jax.shard_map(
        shards, mesh=finer, in_specs=in_specs, out_specs=out_specs, check_vma=False
    )
```

```python
import functools

import jax
import jax.numpy as jnp
from jax import lax
from jax.experimental import pallas as pl
from jax.experimental.pallas import tpu as pltpu
from jax.sharding import Mesh
from jax.sharding import PartitionSpec as P

HD = 128
HALF = HD // 2
X = ("x2", "x1", "x0")
Y = ("y2", "y1", "y0")
MESH = X + Y
FAR = ("x2", "x1", "y2", "y1")
SIDE = 8
FAR_COUNT = 16
norm_epsilon = 1e-05
rope_theta = 500000.0
MIB = 1024 * 1024


def frequencies():
    return rope_theta ** (-(2.0 * jnp.arange(HALF, dtype=jnp.float32)) / HD)


def position_tables(segment_row, freqs):
    row_length = segment_row.shape[0]
    indices = jnp.arange(row_length, dtype=jnp.int32)
    same = segment_row[None, :] == segment_row[:, None]
    first_index = jnp.min(jnp.where(same, indices[None, :], row_length), axis=1)
    positions = (indices - first_index).astype(jnp.float32)
    angles = positions[:, None] * freqs[None, :]
    cosine, sine = jnp.cos(angles), jnp.sin(angles)
    allowed = (indices[None, :] <= indices[:, None]) & same
    return (
        jnp.concatenate([cosine, cosine], axis=1),
        jnp.concatenate([-sine, sine], axis=1),
        allowed.astype(jnp.float32),
    )


STAGES = (
    ((0, 0, 0),),
    ((1, 0, 0), (1, 0, 8), (0, 1, 0), (0, 1, 8)),
    ((1, 1, 0), (1, 1, 8)),
)
STEP = 4


def for_chunks(buffers, layout, body, carry, unrolled=False):
    px, py = lax.axis_index("x0"), lax.axis_index("y0")
    for ref, (turn_x, turn_y, first) in zip(buffers, layout, strict=True):
        base = SIDE * jnp.where(turn_x == 1, 1 - px, px) + jnp.where(turn_y == 1, 1 - py, py)
        base += 2 * SIDE * (first // STEP)

        def chunk(i, carry, ref=ref, base=base):
            place = base + 2 * SIDE * i
            return body([(ref[i * STEP + k], place + 2 * k) for k in range(STEP)], carry)

        count = ref.shape[0] // STEP
        if unrolled:
            for i in range(count):
                carry = chunk(i, carry)
        else:
            carry = lax.fori_loop(0, count, chunk, carry)
    return carry


def at(place, width):
    return pl.ds(pl.multiple_of(place * width, width), width)


def is_other(section):
    return lax.axis_index("section") != section


def weight_rows(second, own, other, chunk, width):
    parts = []
    for _, place in chunk:
        parts.append(jnp.where(second, other[at(place, width), :], own[at(place, width), :]))
    return jnp.concatenate(parts, axis=0)


def squares_of(buffers, total):
    for ref in buffers:
        for j in range(ref.shape[0]):
            part = ref[j].astype(jnp.float32)
            total += part * part
    return total


def squares_kernel(*refs):
    buffers, total = refs[:-1], refs[-1]
    total[...] = squares_of(buffers, jnp.zeros(total.shape, jnp.float32))


def project_kernel(section, layout, late, squares, *rest):
    gain_own, gain_other, own, other, kv_own, kv_other, cosine, sine = rest[:8]
    buffers, (query, keyval) = rest[8:-2], rest[-2:]
    second = is_other(section)
    rows, width = query.shape
    columns = kv_own.shape[0]
    features = width * gain_own.shape[0]
    total = squares_of(buffers[-late:], squares[...])
    scale = lax.rsqrt(jnp.sum(total, axis=1, keepdims=True) / features + norm_epsilon)

    def body(chunk, carry):
        q_sum, kv_sum = carry
        normed, kv_parts = [], []
        for part, place in chunk:
            gain = jnp.where(second, gain_other[place], gain_own[place])
            normed.append((part.astype(jnp.float32) * scale * gain).astype(jnp.bfloat16))
            span = at(place, width)
            kv_parts.append(jnp.where(second, kv_other[:, span], kv_own[:, span]))
        normed = jnp.concatenate(normed, axis=1)
        weight = weight_rows(second, own, other, chunk, width)
        q_sum += jnp.dot(normed, weight, preferred_element_type=jnp.float32)
        kv_sum += lax.dot_general(
            normed,
            jnp.concatenate(kv_parts, axis=1),
            (((1,), (1,)), ((), ())),
            preferred_element_type=jnp.float32,
        )
        return q_sum, kv_sum

    zero = jnp.zeros((rows, width), jnp.float32), jnp.zeros((rows, columns), jnp.float32)
    q_sum, kv_sum = for_chunks(buffers, layout, body, zero, unrolled=True)
    turned = jnp.concatenate([q_sum[:, HALF:], q_sum[:, :HALF]], axis=1)
    query[...] = (q_sum * cosine[...] + turned * sine[...]).astype(query.dtype)
    flat = kv_sum.T.astype(keyval.dtype)
    keyval[...] = jnp.broadcast_to(flat[None], keyval.shape)


def attend_kernel(query, keyval, cosine, sine, allowed, attended):
    keys = keyval[:HD, :].astype(jnp.float32)
    turned = jnp.concatenate([keys[HALF:], keys[:HALF]], axis=0)
    keys = (keys * cosine[...].T + turned * sine[...].T).astype(jnp.bfloat16)
    scores = jnp.dot(query[...], keys, preferred_element_type=jnp.float32) * HD ** (-0.5)
    masked = jnp.where(allowed[...] > 0.0, scores, -1e30)
    highest = jnp.max(masked, axis=1, keepdims=True)
    raised = jnp.exp(masked - highest)
    probs = (raised / jnp.sum(raised, axis=1, keepdims=True)).astype(jnp.bfloat16)
    out = lax.dot_general(
        probs, keyval[HD:, :], (((1,), (1,)), ((), ())), preferred_element_type=jnp.float32
    ).astype(jnp.bfloat16)
    attended[...] = jnp.broadcast_to(out[None], attended.shape)


def mix_kernel(section, layout, earlier, own, other, before, *rest):
    past, rest = rest[:earlier], rest[earlier:]
    buffers, outs = rest[: len(layout)], rest[len(layout) :]
    second = is_other(section)
    width = before.shape[1]

    def body(chunk, mixed):
        weight = weight_rows(second, own, other, chunk, width)
        joined = jnp.concatenate([part for part, _ in chunk], axis=1)
        return mixed + jnp.dot(joined, weight, preferred_element_type=jnp.float32)

    mixed = for_chunks(buffers, layout, body, before[...].astype(jnp.float32))
    out = mixed.astype(outs[0].dtype)
    if past:
        lower = lax.axis_index("section") == 0
        outs[0][...] = jnp.where(lower, past[0][...], out)
        outs[1][...] = jnp.where(lower, out, past[0][...])
        return
    outs[0][...] = out
    if len(outs) > 1:
        outs[1][...] = jnp.broadcast_to(out[None], outs[1].shape)


def start_kernel(inputs, segments, current, copies, segment_row):
    me = lax.axis_index("section")
    block = inputs[me]
    current[...] = block
    copies[...] = jnp.broadcast_to(block[None], copies.shape)
    segment_row[...] = jnp.where(me == 0, segments[0:1, :], segments[1:2, :])


def place_kernel(mine, theirs, result):
    me = lax.axis_index("section")
    result[me] = mine[...]
    result[1 - me] = theirs[...]


def call(kernel, outs, limit, *args):
    vmem = pl.BlockSpec(memory_space=pltpu.VMEM)
    return pl.pallas_call(
        kernel,
        out_shape=outs,
        in_specs=[vmem] * len(args),
        out_specs=jax.tree.map(lambda _: vmem, outs),
        compiler_params=pltpu.CompilerParams(vmem_limit_bytes=limit * MIB),
    )(*args)


def from_neighbour(block, dx, dy):
    pairs = []
    for x in range(SIDE):
        for y in range(SIDE):
            there = (x + dx) % SIDE * SIDE + (y + dy) % SIDE
            pairs.append((there, x * SIDE + y))
    return lax.ppermute(block, MESH, pairs)


def far_stage(copies):
    return lax.all_to_all(copies, FAR, 0, 0, tiled=True)


def near_stage(own):
    low, high = own[:8], own[8:]
    xa, xb = from_neighbour(low, 1, 0), from_neighbour(high, -1, 0)
    ya, yb = from_neighbour(low, 0, 1), from_neighbour(high, 0, -1)
    da, db = from_neighbour(xa, 0, 1), from_neighbour(xb, 0, -1)
    return (own,), (xa, xb, ya, yb), (da, db)


def shards(inputs, segments, gains, w_query, w_keyval, w_output):
    _, rows, width = inputs.shape
    sections = lax.axis_size("section")
    ring = lax.axis_size(Y)
    swap = [(0, 1), (1, 0)]
    own = [w_query[0, 0], w_keyval[0, 0].T, w_output[0, 0]]
    gain = gains[0].astype(jnp.float32).reshape(-1, 1, width)
    other = []
    for w in own:
        other.append(lax.ppermute(w, "section", swap))
    other_gain = lax.ppermute(gain, "section", swap)
    shape = jax.ShapeDtypeStruct
    bf16 = functools.partial(shape, dtype=jnp.bfloat16)
    f32 = functools.partial(shape, dtype=jnp.float32)
    columns = own[1].shape[0]
    outs = (bf16((rows, width)), bf16((FAR_COUNT, rows, width)), shape((1, rows), jnp.int32))
    current, copies, segment_row = call(start_kernel, outs, 4, inputs, segments)
    copies, segment_row, freqs = lax.optimization_barrier((copies, segment_row, frequencies()))
    stages = len(STAGES)
    for s in range(sections):
        far = far_stage(copies)
        if s == 0:
            far, segment_row = lax.optimization_barrier((far, segment_row))
            cosine, sine, allowed = position_tables(segment_row[0], freqs)
        near = near_stage(far)
        squares = call(squares_kernel, f32((rows, width)), 4, *near[0], *near[1])
        squares, cosine, sine, allowed = lax.optimization_barrier(
            (squares, cosine, sine, allowed)
        )
        weights = (gain, other_gain, own[0], other[0], own[1], other[1])
        kernel = functools.partial(project_kernel, s, sum(STAGES, ()), len(STAGES[-1]))
        outs = (bf16((rows, width)), bf16((ring, columns, rows)))
        query, keyval = call(kernel, outs, 10, squares, *weights, cosine, sine, *sum(near, ()))
        keyval = lax.all_to_all(keyval, Y, 0, 0, tiled=True).reshape(-1, rows)
        attended = call(
            attend_kernel, bf16((FAR_COUNT, rows, width)), 4, query, keyval, cosine, sine, allowed
        )
        near = near_stage(far_stage(attended))
        partial, end = current, s + 1 == sections
        for k, (group, layout) in enumerate(zip(near, STAGES, strict=True)):
            outs, past = (f32((rows, width)),), ()
            if k == stages - 1:
                outs = (bf16((rows, width)),)
                past = (current,) if end else ()
                outs += (bf16((rows, width)),) if end else (bf16((FAR_COUNT, rows, width)),)
            kernel = functools.partial(mix_kernel, s, layout, len(past))
            partial, *extra = call(kernel, outs, 10, own[2], other[2], partial, *past, *group)
        current, copies = partial, extra[0]
    theirs = lax.ppermute(copies, "section", swap)
    return call(place_kernel, bf16((sections, rows, width)), 4, current, theirs)[None]


def solution(mesh):
    finer = Mesh(
        mesh.devices.reshape(mesh.shape["groups"], mesh.shape["section"], *([2] * 6)),
        ("groups", "section") + MESH,
    )
    in_specs = (
        P("groups", None, MESH),
        P("groups", None),
        P("section", None, None),
        P("section", None, None, MESH),
        P("section", None, None, MESH),
        P("section", None, None, MESH),
    )
    out_specs = P("section", "groups", None, MESH)

    return jax.shard_map(
        shards, mesh=finer, in_specs=in_specs, out_specs=out_specs, check_vma=False
    )
```

```python
import functools

import jax
import jax.numpy as jnp
from jax import lax
from jax.experimental import pallas as pl
from jax.experimental.pallas import tpu as pltpu
from jax.sharding import Mesh
from jax.sharding import PartitionSpec as P

HD = 128
HALF = HD // 2
X = ("x2", "x1", "x0")
Y = ("y2", "y1", "y0")
MESH = X + Y
FAR = ("x2", "x1", "y2", "y1")
SIDE = 8
FAR_COUNT = 16
norm_epsilon = 1e-05
rope_theta = 500000.0
MIB = 1024 * 1024


def frequencies():
    return rope_theta ** (-(2.0 * jnp.arange(HALF, dtype=jnp.float32)) / HD)


def position_tables(segment_row, freqs):
    row_length = segment_row.shape[0]
    indices = jnp.arange(row_length, dtype=jnp.int32)
    same = segment_row[None, :] == segment_row[:, None]
    first_index = jnp.min(jnp.where(same, indices[None, :], row_length), axis=1)
    positions = (indices - first_index).astype(jnp.float32)
    angles = positions[:, None] * freqs[None, :]
    cosine, sine = jnp.cos(angles), jnp.sin(angles)
    allowed = (indices[None, :] <= indices[:, None]) & same
    return (
        jnp.concatenate([cosine, cosine], axis=1),
        jnp.concatenate([-sine, sine], axis=1),
        allowed.astype(jnp.float32),
    )


STAGES = (
    ((0, 0, 0),),
    ((1, 0, 0), (1, 0, 8), (0, 1, 0), (0, 1, 8)),
    ((1, 1, 0), (1, 1, 8)),
)
STEP = 4


def for_chunks(buffers, layout, body, carry, unrolled=False):
    px, py = lax.axis_index("x0"), lax.axis_index("y0")
    for ref, (turn_x, turn_y, first) in zip(buffers, layout, strict=True):
        base = SIDE * jnp.where(turn_x == 1, 1 - px, px) + jnp.where(turn_y == 1, 1 - py, py)
        base += 2 * SIDE * (first // STEP)

        def chunk(i, carry, ref=ref, base=base):
            place = base + 2 * SIDE * i
            return body([(ref[i * STEP + k], place + 2 * k) for k in range(STEP)], carry)

        count = ref.shape[0] // STEP
        if unrolled:
            for i in range(count):
                carry = chunk(i, carry)
        else:
            carry = lax.fori_loop(0, count, chunk, carry)
    return carry


def at(place, width):
    return pl.ds(pl.multiple_of(place * width, width), width)


def is_other(section):
    return lax.axis_index("section") != section


def weight_rows(second, own, other, chunk, width):
    parts = []
    for _, place in chunk:
        parts.append(jnp.where(second, other[at(place, width), :], own[at(place, width), :]))
    return jnp.concatenate(parts, axis=0)


def squares_of(buffers, total):
    for ref in buffers:
        for j in range(ref.shape[0]):
            part = ref[j].astype(jnp.float32)
            total += part * part
    return total


def squares_kernel(*refs):
    buffers, total = refs[:-1], refs[-1]
    total[...] = squares_of(buffers, jnp.zeros(total.shape, jnp.float32))


def project_kernel(section, layout, late, squares, *rest):
    gain_own, gain_other, own, other, kv_own, kv_other, cosine, sine = rest[:8]
    buffers, (query, keyval) = rest[8:-2], rest[-2:]
    second = is_other(section)
    rows, width = query.shape
    columns = kv_own.shape[0]
    features = gain_own.shape[1]
    total = squares_of(buffers[-late:], squares[...])
    scale = lax.rsqrt(jnp.sum(total, axis=1, keepdims=True) / features + norm_epsilon)

    def body(chunk, carry):
        q_sum, kv_sum = carry
        normed, kv_parts = [], []
        for part, place in chunk:
            span = at(place, width)
            gain = jnp.where(second, gain_other[:, span], gain_own[:, span]).astype(jnp.float32)
            normed.append((part.astype(jnp.float32) * scale * gain).astype(jnp.bfloat16))
            kv_parts.append(jnp.where(second, kv_other[:, span], kv_own[:, span]))
        normed = jnp.concatenate(normed, axis=1)
        weight = weight_rows(second, own, other, chunk, width)
        q_sum += jnp.dot(normed, weight, preferred_element_type=jnp.float32)
        kv_sum += lax.dot_general(
            normed,
            jnp.concatenate(kv_parts, axis=1),
            (((1,), (1,)), ((), ())),
            preferred_element_type=jnp.float32,
        )
        return q_sum, kv_sum

    zero = jnp.zeros((rows, width), jnp.float32), jnp.zeros((rows, columns), jnp.float32)
    q_sum, kv_sum = for_chunks(buffers, layout, body, zero, unrolled=True)
    turned = jnp.concatenate([q_sum[:, HALF:], q_sum[:, :HALF]], axis=1)
    query[...] = (q_sum * cosine[...] + turned * sine[...]).astype(query.dtype)
    flat = kv_sum.T.astype(keyval.dtype)
    keyval[...] = jnp.broadcast_to(flat[None], keyval.shape)


def attend_kernel(query, keyval, cosine, sine, allowed, attended):
    keys = keyval[:HD, :].astype(jnp.float32)
    turned = jnp.concatenate([keys[HALF:], keys[:HALF]], axis=0)
    keys = (keys * cosine[...].T + turned * sine[...].T).astype(jnp.bfloat16)
    scores = jnp.dot(query[...], keys, preferred_element_type=jnp.float32) * HD ** (-0.5)
    masked = jnp.where(allowed[...] > 0.0, scores, -1e30)
    highest = jnp.max(masked, axis=1, keepdims=True)
    raised = jnp.exp(masked - highest)
    probs = (raised / jnp.sum(raised, axis=1, keepdims=True)).astype(jnp.bfloat16)
    out = lax.dot_general(
        probs, keyval[HD:, :], (((1,), (1,)), ((), ())), preferred_element_type=jnp.float32
    ).astype(jnp.bfloat16)
    attended[...] = jnp.broadcast_to(out[None], attended.shape)


def mix_kernel(section, layout, earlier, own, other, before, *rest):
    past, rest = rest[:earlier], rest[earlier:]
    buffers, outs = rest[: len(layout)], rest[len(layout) :]
    second = is_other(section)
    width = before.shape[1]

    def body(chunk, mixed):
        weight = weight_rows(second, own, other, chunk, width)
        joined = jnp.concatenate([part for part, _ in chunk], axis=1)
        return mixed + jnp.dot(joined, weight, preferred_element_type=jnp.float32)

    mixed = for_chunks(buffers, layout, body, before[...].astype(jnp.float32))
    out = mixed.astype(outs[0].dtype)
    if past:
        lower = lax.axis_index("section") == 0
        outs[0][...] = jnp.where(lower, past[0][...], out)
        outs[1][...] = jnp.where(lower, out, past[0][...])
        return
    outs[0][...] = out
    if len(outs) > 1:
        outs[1][...] = jnp.broadcast_to(out[None], outs[1].shape)


def start_kernel(inputs, segments, current, copies, segment_row, both, sems):
    me = lax.axis_index("section")
    fetch = pltpu.make_async_copy(inputs.at[me], current, sems.at[0])
    fetch_rows = pltpu.make_async_copy(segments, both, sems.at[1])
    fetch.start()
    fetch_rows.start()
    fetch_rows.wait()
    segment_row[...] = jnp.where(me == 0, both[0:1, :], both[1:2, :])
    fetch.wait()
    copies[...] = jnp.broadcast_to(current[...][None], copies.shape)


def place_kernel(mine, theirs, result):
    me = lax.axis_index("section")
    result[me] = mine[...]
    result[1 - me] = theirs[...]


def call(kernel, outs, limit, *args):
    vmem = pl.BlockSpec(memory_space=pltpu.VMEM)
    return pl.pallas_call(
        kernel,
        out_shape=outs,
        in_specs=[vmem] * len(args),
        out_specs=jax.tree.map(lambda _: vmem, outs),
        compiler_params=pltpu.CompilerParams(vmem_limit_bytes=limit * MIB),
    )(*args)


def from_neighbour(block, dx, dy):
    pairs = []
    for x in range(SIDE):
        for y in range(SIDE):
            there = (x + dx) % SIDE * SIDE + (y + dy) % SIDE
            pairs.append((there, x * SIDE + y))
    return lax.ppermute(block, MESH, pairs)


def far_stage(copies):
    return lax.all_to_all(copies, FAR, 0, 0, tiled=True)


def near_stage(own):
    low, high = own[:8], own[8:]

    xa, xb = from_neighbour(low, 1, 0), from_neighbour(high, -1, 0)
    ya, yb = from_neighbour(low, 0, 1), from_neighbour(high, 0, -1)
    da, db = from_neighbour(xa, 0, 1), from_neighbour(xb, 0, -1)
    return (own,), (xa, xb, ya, yb), (da, db)


def shards(inputs, segments, gains, w_query, w_keyval, w_output):
    _, rows, width = inputs.shape
    sections = lax.axis_size("section")
    ring = lax.axis_size(Y)
    swap = [(0, 1), (1, 0)]
    own = [w_query[0, 0], w_keyval[0, 0].T, w_output[0, 0]]
    other = []
    for w in own:
        other.append(lax.ppermute(w, "section", swap))
    other_gain = lax.ppermute(gains[0], "section", swap)
    shape = jax.ShapeDtypeStruct
    bf16 = functools.partial(shape, dtype=jnp.bfloat16)
    f32 = functools.partial(shape, dtype=jnp.float32)
    columns = own[1].shape[0]
    outs = (bf16((rows, width)), bf16((FAR_COUNT, rows, width)), shape((1, rows), jnp.int32))
    anywhere, vmem = pl.BlockSpec(memory_space=pltpu.HBM), pl.BlockSpec(memory_space=pltpu.VMEM)
    current, copies, segment_row = pl.pallas_call(
        start_kernel,
        out_shape=outs,
        in_specs=[anywhere, anywhere],
        out_specs=(vmem,) * len(outs),
        scratch_shapes=[
            pltpu.VMEM(segments.shape, segments.dtype),
            pltpu.SemaphoreType.DMA((2,)),
        ],
        compiler_params=pltpu.CompilerParams(vmem_limit_bytes=2 * MIB),
    )(*(pltpu.with_memory_space_constraint(a, pltpu.HBM) for a in (inputs, segments)))
    copies, segment_row, freqs = lax.optimization_barrier((copies, segment_row, frequencies()))
    stages = len(STAGES)
    for s in range(sections):
        far = far_stage(copies)
        if s == 0:
            far, segment_row = lax.optimization_barrier((far, segment_row))
            cosine, sine, allowed = position_tables(segment_row[0], freqs)
        near = near_stage(far)
        squares = call(squares_kernel, f32((rows, width)), 4, *near[0], *near[1])
        squares, cosine, sine, allowed = lax.optimization_barrier(
            (squares, cosine, sine, allowed)
        )
        weights = (gains[0], other_gain, own[0], other[0], own[1], other[1])
        kernel = functools.partial(project_kernel, s, sum(STAGES, ()), len(STAGES[-1]))
        outs = (bf16((rows, width)), bf16((ring, columns, rows)))
        query, keyval = call(kernel, outs, 10, squares, *weights, cosine, sine, *sum(near, ()))
        keyval = lax.all_to_all(keyval, Y, 0, 0, tiled=True).reshape(-1, rows)
        attended = call(
            attend_kernel, bf16((FAR_COUNT, rows, width)), 4, query, keyval, cosine, sine, allowed
        )
        near = near_stage(far_stage(attended))
        partial, end = current, s + 1 == sections
        for k, (group, layout) in enumerate(zip(near, STAGES, strict=True)):
            outs, past = (f32((rows, width)),), ()
            if k == stages - 1:
                outs = (bf16((rows, width)),)
                past = (current,) if end else ()
                outs += (bf16((rows, width)),) if end else (bf16((FAR_COUNT, rows, width)),)
            kernel = functools.partial(mix_kernel, s, layout, len(past))
            partial, *extra = call(kernel, outs, 10, own[2], other[2], partial, *past, *group)
        current, copies = partial, extra[0]
    theirs = lax.ppermute(copies, "section", swap)
    return call(place_kernel, bf16((sections, rows, width)), 4, current, theirs)[None]


def solution(mesh):
    finer = Mesh(
        mesh.devices.reshape(mesh.shape["groups"], mesh.shape["section"], *([2] * 6)),
        ("groups", "section") + MESH,
    )
    in_specs = (
        P("groups", None, MESH),
        P("groups", None),
        P("section", None, None),
        P("section", None, None, MESH),
        P("section", None, None, MESH),
        P("section", None, None, MESH),
    )
    out_specs = P("section", "groups", None, MESH)

    return jax.shard_map(
        shards, mesh=finer, in_specs=in_specs, out_specs=out_specs, check_vma=False
    )
```

```python
import functools

import jax
import jax.numpy as jnp
from jax import lax
from jax.experimental import pallas as pl
from jax.experimental.pallas import tpu as pltpu
from jax.sharding import Mesh
from jax.sharding import PartitionSpec as P

HD = 128
HALF = HD // 2
X = ("x2", "x1", "x0")
Y = ("y2", "y1", "y0")
MESH = X + Y
FAR = ("x2", "x1", "y2", "y1")
SIDE = 8
FAR_COUNT = 16
norm_epsilon = 1e-05
rope_theta = 500000.0
MIB = 1024 * 1024


def frequencies():
    return rope_theta ** (-(2.0 * jnp.arange(HALF, dtype=jnp.float32)) / HD)


def position_tables(segment_row, freqs):
    row_length = segment_row.shape[0]
    indices = jnp.arange(row_length, dtype=jnp.int32)
    same = segment_row[None, :] == segment_row[:, None]
    first_index = jnp.min(jnp.where(same, indices[None, :], row_length), axis=1)
    positions = (indices - first_index).astype(jnp.float32)
    angles = positions[:, None] * freqs[None, :]
    cosine, sine = jnp.cos(angles), jnp.sin(angles)
    allowed = (indices[None, :] <= indices[:, None]) & same
    return (
        jnp.concatenate([cosine, cosine], axis=1),
        jnp.concatenate([-sine, sine], axis=1),
        allowed.astype(jnp.float32),
    )


STAGES = (
    ((0, 0),),
    ((1, 1), (1, 0), (0, 1)),
)
STEP = 4


def for_chunks(buffers, layout, body, carry, unrolled=False):
    px, py = lax.axis_index("x0"), lax.axis_index("y0")
    for ref, (turn_x, turn_y) in zip(buffers, layout, strict=True):
        base = SIDE * jnp.where(turn_x == 1, 1 - px, px) + jnp.where(turn_y == 1, 1 - py, py)

        def chunk(i, carry, ref=ref, base=base):
            place = base + 2 * SIDE * i
            return body([(ref[i * STEP + k], place + 2 * k) for k in range(STEP)], carry)

        count = ref.shape[0] // STEP
        if unrolled:
            for i in range(count):
                carry = chunk(i, carry)
        else:
            carry = lax.fori_loop(0, count, chunk, carry)
    return carry


def at(place, width):
    return pl.ds(pl.multiple_of(place * width, width), width)


def is_other(section):
    return lax.axis_index("section") != section


def weight_rows(second, own, other, chunk, width):
    parts = []
    for _, place in chunk:
        parts.append(jnp.where(second, other[at(place, width), :], own[at(place, width), :]))
    return jnp.concatenate(parts, axis=0)


def squares_of(buffers, total):
    for ref in buffers:
        for j in range(ref.shape[0]):
            part = ref[j].astype(jnp.float32)
            total += part * part
    return total


def squares_kernel(own_set, total):
    total[...] = squares_of((own_set,), jnp.zeros(total.shape, jnp.float32))


def project_kernel(section, layout, late, squares, *rest):
    gain_own, gain_other, own, other, kv_own, kv_other, cosine, sine = rest[:8]
    buffers, (query, keyval) = rest[8:-2], rest[-2:]
    second = is_other(section)
    rows, width = query.shape
    columns = kv_own.shape[0]
    features = gain_own.shape[1]
    total = squares_of(buffers[-late:], squares[...])
    scale = lax.rsqrt(jnp.sum(total, axis=1, keepdims=True) / features + norm_epsilon)

    def body(chunk, carry):
        q_sum, kv_sum = carry
        normed, kv_parts = [], []
        for part, place in chunk:
            span = at(place, width)
            gain = jnp.where(second, gain_other[:, span], gain_own[:, span]).astype(jnp.float32)
            normed.append((part.astype(jnp.float32) * scale * gain).astype(jnp.bfloat16))
            kv_parts.append(jnp.where(second, kv_other[:, span], kv_own[:, span]))
        normed = jnp.concatenate(normed, axis=1)
        weight = weight_rows(second, own, other, chunk, width)
        q_sum += jnp.dot(normed, weight, preferred_element_type=jnp.float32)
        kv_sum += lax.dot_general(
            normed,
            jnp.concatenate(kv_parts, axis=1),
            (((1,), (1,)), ((), ())),
            preferred_element_type=jnp.float32,
        )
        return q_sum, kv_sum

    zero = jnp.zeros((rows, width), jnp.float32), jnp.zeros((rows, columns), jnp.float32)
    q_sum, kv_sum = for_chunks(buffers, layout, body, zero, unrolled=True)
    turned = jnp.concatenate([q_sum[:, HALF:], q_sum[:, :HALF]], axis=1)
    query[...] = (q_sum * cosine[...] + turned * sine[...]).astype(query.dtype)
    flat = kv_sum.T.astype(keyval.dtype)
    keyval[...] = jnp.broadcast_to(flat[None], keyval.shape)


def attend_kernel(query, keyval, cosine, sine, allowed, attended):
    keys = keyval[:HD, :].astype(jnp.float32)
    turned = jnp.concatenate([keys[HALF:], keys[:HALF]], axis=0)
    keys = (keys * cosine[...].T + turned * sine[...].T).astype(jnp.bfloat16)
    scores = jnp.dot(query[...], keys, preferred_element_type=jnp.float32) * HD ** (-0.5)
    masked = jnp.where(allowed[...] > 0.0, scores, -1e30)
    highest = jnp.max(masked, axis=1, keepdims=True)
    raised = jnp.exp(masked - highest)
    probs = (raised / jnp.sum(raised, axis=1, keepdims=True)).astype(jnp.bfloat16)
    out = lax.dot_general(
        probs, keyval[HD:, :], (((1,), (1,)), ((), ())), preferred_element_type=jnp.float32
    ).astype(jnp.bfloat16)
    attended[...] = jnp.broadcast_to(out[None], attended.shape)


def mix_kernel(section, layout, earlier, own, other, before, *rest):
    past, rest = rest[:earlier], rest[earlier:]
    buffers, outs = rest[: len(layout)], rest[len(layout) :]
    second = is_other(section)
    width = before.shape[1]

    def body(chunk, mixed):
        weight = weight_rows(second, own, other, chunk, width)
        joined = jnp.concatenate([part for part, _ in chunk], axis=1)
        return mixed + jnp.dot(joined, weight, preferred_element_type=jnp.float32)

    mixed = before[...].astype(jnp.float32)
    mixed = for_chunks(buffers, layout, body, mixed, unrolled=len(layout) > 1)
    out = mixed.astype(outs[0].dtype)
    if past:
        lower = lax.axis_index("section") == 0
        outs[0][...] = jnp.where(lower, past[0][...], out)
        outs[1][...] = jnp.where(lower, out, past[0][...])
        return
    outs[0][...] = out
    if len(outs) > 1:
        outs[1][...] = jnp.broadcast_to(out[None], outs[1].shape)


def start_kernel(
    inputs, segments, kv, gains, current, copies, segment_row, kv_out, gains_out, both, sems
):
    me = lax.axis_index("section")
    moves = ((inputs.at[me], current), (segments, both), (kv, kv_out), (gains, gains_out))
    fetches = [pltpu.make_async_copy(a, b, sems.at[k]) for k, (a, b) in enumerate(moves)]
    for fetch in fetches:
        fetch.start()
    fetches[0].wait()
    copies[...] = jnp.broadcast_to(current[...][None], copies.shape)
    fetches[1].wait()
    segment_row[...] = jnp.where(me == 0, both[0:1, :], both[1:2, :])
    fetches[2].wait()
    fetches[3].wait()


def place_kernel(mine, theirs, result):
    me = lax.axis_index("section")
    result[me] = mine[...]
    result[1 - me] = theirs[...]


def call(kernel, outs, limit, *args):
    vmem = pl.BlockSpec(memory_space=pltpu.VMEM)
    return pl.pallas_call(
        kernel,
        out_shape=outs,
        in_specs=[vmem] * len(args),
        out_specs=jax.tree.map(lambda _: vmem, outs),
        compiler_params=pltpu.CompilerParams(vmem_limit_bytes=limit * MIB),
    )(*args)


def from_neighbour(block, dx, dy):
    pairs = []
    for x in range(SIDE):
        for y in range(SIDE):
            there = (x + dx) % SIDE * SIDE + (y + dy) % SIDE
            pairs.append((there, x * SIDE + y))
    return lax.ppermute(block, MESH, pairs)


def far_stage(copies):
    return lax.all_to_all(copies, FAR, 0, 0, tiled=True)


def near_stage(own):
    def hop(dx, dy):
        return from_neighbour(own, dx, dy)

    return (own,), (hop(-1, -1), hop(1, 0), hop(0, 1))


def shards(inputs, segments, gains, w_query, w_keyval, w_output):
    _, rows, width = inputs.shape
    sections = lax.axis_size("section")
    ring = lax.axis_size(Y)
    swap = [(0, 1), (1, 0)]
    own = [w_query[0, 0], w_keyval[0, 0].T, w_output[0, 0]]
    other = []
    for w in own:
        other.append(lax.ppermute(w, "section", swap))
    other_gain = lax.ppermute(gains[0], "section", swap)
    shape = jax.ShapeDtypeStruct
    bf16 = functools.partial(shape, dtype=jnp.bfloat16)
    f32 = functools.partial(shape, dtype=jnp.float32)
    columns = own[1].shape[0]
    outs = (bf16((rows, width)), bf16((FAR_COUNT, rows, width)), shape((1, rows), jnp.int32))
    outs += (bf16(own[1].shape), bf16(gains[0].shape))
    sources = (inputs, segments, own[1], gains[0])
    anywhere, vmem = pl.BlockSpec(memory_space=pltpu.HBM), pl.BlockSpec(memory_space=pltpu.VMEM)
    current, copies, segment_row, own[1], gain = pl.pallas_call(
        start_kernel,
        out_shape=outs,
        in_specs=[anywhere] * len(sources),
        out_specs=(vmem,) * len(outs),
        scratch_shapes=[
            pltpu.VMEM(segments.shape, segments.dtype),
            pltpu.SemaphoreType.DMA((len(sources),)),
        ],
        compiler_params=pltpu.CompilerParams(vmem_limit_bytes=4 * MIB),
    )(*(pltpu.with_memory_space_constraint(a, pltpu.HBM) for a in sources))
    copies, segment_row, freqs = lax.optimization_barrier((copies, segment_row, frequencies()))
    stages = len(STAGES)
    for s in range(sections):
        far = far_stage(copies)
        if s == 0:
            far, segment_row = lax.optimization_barrier((far, segment_row))
            cosine, sine, allowed = position_tables(segment_row[0], freqs)
        near = near_stage(far)
        squares = call(squares_kernel, f32((rows, width)), 4, *near[0])
        squares, cosine, sine, allowed = lax.optimization_barrier(
            (squares, cosine, sine, allowed)
        )
        weights = (gain, other_gain, own[0], other[0], own[1], other[1])
        kernel = functools.partial(project_kernel, s, sum(STAGES, ()), len(STAGES[-1]))
        outs = (bf16((rows, width)), bf16((ring, columns, rows)))
        query, keyval = call(kernel, outs, 10, squares, *weights, cosine, sine, *sum(near, ()))
        keyval = lax.all_to_all(keyval, Y, 0, 0, tiled=True).reshape(-1, rows)
        attended = call(
            attend_kernel, bf16((FAR_COUNT, rows, width)), 4, query, keyval, cosine, sine, allowed
        )
        near = near_stage(far_stage(attended))
        partial, end = current, s + 1 == sections
        for k, (group, layout) in enumerate(zip(near, STAGES, strict=True)):
            outs, past = (f32((rows, width)),), ()
            if k == stages - 1:
                outs = (bf16((rows, width)),)
                past = (current,) if end else ()
                outs += (bf16((rows, width)),) if end else (bf16((FAR_COUNT, rows, width)),)
            kernel = functools.partial(mix_kernel, s, layout, len(past))
            partial, *extra = call(kernel, outs, 10, own[2], other[2], partial, *past, *group)
        current, copies = partial, extra[0]
    theirs = lax.ppermute(copies, "section", swap)
    return call(place_kernel, bf16((sections, rows, width)), 4, current, theirs)[None]


def solution(mesh):
    finer = Mesh(
        mesh.devices.reshape(mesh.shape["groups"], mesh.shape["section"], *([2] * 6)),
        ("groups", "section") + MESH,
    )
    in_specs = (
        P("groups", None, MESH),
        P("groups", None),
        P("section", None, None),
        P("section", None, None, MESH),
        P("section", None, None, MESH),
        P("section", None, None, MESH),
    )
    out_specs = P("section", "groups", None, MESH)

    return jax.shard_map(
        shards, mesh=finer, in_specs=in_specs, out_specs=out_specs, check_vma=False
    )
```

```python
import functools

import jax
import jax.numpy as jnp
from jax import lax
from jax.experimental import pallas as pl
from jax.experimental.pallas import tpu as pltpu
from jax.sharding import Mesh
from jax.sharding import PartitionSpec as P

HD = 128
HALF = HD // 2
X = ("x2", "x1", "x0")
Y = ("y2", "y1", "y0")
MESH = X + Y
SIDE = 8
FAR_COUNT = 16
norm_epsilon = 1e-05
rope_theta = 500000.0
MIB = 1024 * 1024


def frequencies():
    return rope_theta ** (-(2.0 * jnp.arange(HALF, dtype=jnp.float32)) / HD)


def position_tables(segment_row, freqs):
    row_length = segment_row.shape[0]
    indices = jnp.arange(row_length, dtype=jnp.int32)
    same = segment_row[None, :] == segment_row[:, None]
    first_index = jnp.min(jnp.where(same, indices[None, :], row_length), axis=1)
    positions = (indices - first_index).astype(jnp.float32)
    angles = positions[:, None] * freqs[None, :]
    cosine, sine = jnp.cos(angles), jnp.sin(angles)
    allowed = (indices[None, :] <= indices[:, None]) & same
    return (
        jnp.concatenate([cosine, cosine], axis=1),
        jnp.concatenate([-sine, sine], axis=1),
        allowed.astype(jnp.float32),
    )


STAGES = ((0,), (1, 3, 2))
STEP = 4


def colour_groups(devices):
    groups = [[] for _ in range(STEP)]
    for place in range(devices):
        groups[(place // SIDE + 2 * (place % SIDE)) % STEP].append(place)
    return groups


def for_chunks(buffers, layout, body, carry, unrolled=False):
    for ref, turn in zip(buffers, layout, strict=True):
        odd, half = lax.axis_index("x0"), lax.axis_index("x1") + lax.axis_index("y0")
        colour = odd + 2 * half + turn
        odd, half = colour % 2, colour // 2

        def chunk(i, carry, ref=ref, odd=odd, half=half):
            place = SIDE * odd + 2 * SIDE * i + (half + i) % 2
            return body([(ref[i * STEP + k], place + 2 * k) for k in range(STEP)], carry)

        count = ref.shape[0] // STEP
        if unrolled:
            for i in range(count):
                carry = chunk(i, carry)
        else:
            carry = lax.fori_loop(0, count, chunk, carry)
    return carry


def at(place, width):
    return pl.ds(pl.multiple_of(place * width, width), width)


def is_other(section):
    return lax.axis_index("section") != section


def weight_rows(second, own, other, chunk, width):
    parts = []
    for _, place in chunk:
        parts.append(jnp.where(second, other[at(place, width), :], own[at(place, width), :]))
    return jnp.concatenate(parts, axis=0)


def squares_of(buffers, total):
    for ref in buffers:
        for j in range(ref.shape[0]):
            part = ref[j].astype(jnp.float32)
            total += part * part
    return total


def squares_kernel(own_set, total):
    total[...] = squares_of((own_set,), jnp.zeros(total.shape, jnp.float32))


def project_kernel(section, layout, late, squares, *rest):
    gain_own, gain_other, own, other, kv_own, kv_other, cosine, sine = rest[:8]
    buffers, (query, keyval) = rest[8:-2], rest[-2:]
    second = is_other(section)
    rows, width = query.shape
    columns = kv_own.shape[0]
    features = gain_own.shape[1]
    total = squares_of(buffers[-late:], squares[...])
    scale = lax.rsqrt(jnp.sum(total, axis=1, keepdims=True) / features + norm_epsilon)

    def body(chunk, carry):
        q_sum, kv_sum = carry
        normed, kv_parts = [], []
        for part, place in chunk:
            span = at(place, width)
            gain = jnp.where(second, gain_other[:, span], gain_own[:, span]).astype(jnp.float32)
            normed.append((part.astype(jnp.float32) * scale * gain).astype(jnp.bfloat16))
            kv_parts.append(jnp.where(second, kv_other[:, span], kv_own[:, span]))
        normed = jnp.concatenate(normed, axis=1)
        weight = weight_rows(second, own, other, chunk, width)
        q_sum += jnp.dot(normed, weight, preferred_element_type=jnp.float32)
        kv_sum += lax.dot_general(
            normed,
            jnp.concatenate(kv_parts, axis=1),
            (((1,), (1,)), ((), ())),
            preferred_element_type=jnp.float32,
        )
        return q_sum, kv_sum

    zero = jnp.zeros((rows, width), jnp.float32), jnp.zeros((rows, columns), jnp.float32)
    q_sum, kv_sum = for_chunks(buffers, layout, body, zero, unrolled=True)
    turned = jnp.concatenate([q_sum[:, HALF:], q_sum[:, :HALF]], axis=1)
    query[...] = (q_sum * cosine[...] + turned * sine[...]).astype(query.dtype)
    flat = kv_sum.T.astype(keyval.dtype)
    keyval[...] = jnp.broadcast_to(flat[None], keyval.shape)


def attend_kernel(query, keyval, cosine, sine, allowed, attended):
    keys = keyval[:HD, :].astype(jnp.float32)
    turned = jnp.concatenate([keys[HALF:], keys[:HALF]], axis=0)
    keys = (keys * cosine[...].T + turned * sine[...].T).astype(jnp.bfloat16)
    scores = jnp.dot(query[...], keys, preferred_element_type=jnp.float32) * HD ** (-0.5)
    masked = jnp.where(allowed[...] > 0.0, scores, -1e30)
    highest = jnp.max(masked, axis=1, keepdims=True)
    raised = jnp.exp(masked - highest)
    probs = (raised / jnp.sum(raised, axis=1, keepdims=True)).astype(jnp.bfloat16)
    out = lax.dot_general(
        probs, keyval[HD:, :], (((1,), (1,)), ((), ())), preferred_element_type=jnp.float32
    ).astype(jnp.bfloat16)
    attended[...] = jnp.broadcast_to(out[None], attended.shape)


def mix_kernel(section, layout, earlier, own, other, before, *rest):
    past, rest = rest[:earlier], rest[earlier:]
    buffers, outs = rest[: len(layout)], rest[len(layout) :]
    second = is_other(section)
    width = before.shape[1]

    def body(chunk, mixed):
        weight = weight_rows(second, own, other, chunk, width)
        joined = jnp.concatenate([part for part, _ in chunk], axis=1)
        return mixed + jnp.dot(joined, weight, preferred_element_type=jnp.float32)

    mixed = before[...].astype(jnp.float32)
    mixed = for_chunks(buffers, layout, body, mixed, unrolled=len(layout) > 1)
    out = mixed.astype(outs[0].dtype)
    if past:
        lower = lax.axis_index("section") == 0
        outs[0][...] = jnp.where(lower, past[0][...], out)
        outs[1][...] = jnp.where(lower, out, past[0][...])
        return
    outs[0][...] = out
    if len(outs) > 1:
        outs[1][...] = jnp.broadcast_to(out[None], outs[1].shape)


def start_kernel(
    inputs, segments, kv, gains, current, copies, segment_row, kv_out, gains_out, both, sems
):
    me = lax.axis_index("section")
    moves = ((inputs.at[me], current), (segments, both), (kv, kv_out), (gains, gains_out))
    fetches = [pltpu.make_async_copy(a, b, sems.at[k]) for k, (a, b) in enumerate(moves)]
    for fetch in fetches:
        fetch.start()
    fetches[0].wait()
    copies[...] = jnp.broadcast_to(current[...][None], copies.shape)
    fetches[1].wait()
    segment_row[...] = jnp.where(me == 0, both[0:1, :], both[1:2, :])
    fetches[2].wait()
    fetches[3].wait()


def place_kernel(mine, theirs, result):
    me = lax.axis_index("section")
    result[me] = mine[...]
    result[1 - me] = theirs[...]


def call(kernel, outs, limit, *args):
    vmem = pl.BlockSpec(memory_space=pltpu.VMEM)
    return pl.pallas_call(
        kernel,
        out_shape=outs,
        in_specs=[vmem] * len(args),
        out_specs=jax.tree.map(lambda _: vmem, outs),
        compiler_params=pltpu.CompilerParams(vmem_limit_bytes=limit * MIB),
    )(*args)


def from_neighbour(block, dx, dy):
    pairs = []
    for x in range(SIDE):
        for y in range(SIDE):
            there = (x + dx) % SIDE * SIDE + (y + dy) % SIDE
            pairs.append((there, x * SIDE + y))
    return lax.ppermute(block, MESH, pairs)


def far_stage(copies):
    groups = colour_groups(lax.axis_size(MESH))
    return lax.all_to_all(copies, MESH, 0, 0, axis_index_groups=groups, tiled=True)


def near_stage(own):
    def hop(dx, dy):
        return from_neighbour(own, dx, dy)

    return (own,), (hop(1, 0), hop(-1, 0), hop(0, 1))


def shards(inputs, segments, gains, w_query, w_keyval, w_output):
    _, rows, width = inputs.shape
    sections = lax.axis_size("section")
    ring = lax.axis_size(Y)
    swap = [(0, 1), (1, 0)]
    own = [w_query[0, 0], w_keyval[0, 0].T, w_output[0, 0]]
    other = []
    for w in own:
        other.append(lax.ppermute(w, "section", swap))
    other_gain = lax.ppermute(gains[0], "section", swap)
    shape = jax.ShapeDtypeStruct
    bf16 = functools.partial(shape, dtype=jnp.bfloat16)
    f32 = functools.partial(shape, dtype=jnp.float32)
    columns = own[1].shape[0]
    outs = (bf16((rows, width)), bf16((FAR_COUNT, rows, width)), shape((1, rows), jnp.int32))
    outs += (bf16(own[1].shape), bf16(gains[0].shape))
    sources = (inputs, segments, own[1], gains[0])
    anywhere, vmem = pl.BlockSpec(memory_space=pltpu.HBM), pl.BlockSpec(memory_space=pltpu.VMEM)
    current, copies, segment_row, own[1], gain = pl.pallas_call(
        start_kernel,
        out_shape=outs,
        in_specs=[anywhere] * len(sources),
        out_specs=(vmem,) * len(outs),
        scratch_shapes=[
            pltpu.VMEM(segments.shape, segments.dtype),
            pltpu.SemaphoreType.DMA((len(sources),)),
        ],
        compiler_params=pltpu.CompilerParams(vmem_limit_bytes=4 * MIB),
    )(*(pltpu.with_memory_space_constraint(a, pltpu.HBM) for a in sources))
    copies, segment_row, freqs = lax.optimization_barrier((copies, segment_row, frequencies()))
    stages = len(STAGES)
    for s in range(sections):
        far = far_stage(copies)
        if s == 0:
            far, segment_row = lax.optimization_barrier((far, segment_row))
            cosine, sine, allowed = position_tables(segment_row[0], freqs)
        near = near_stage(far)
        squares = call(squares_kernel, f32((rows, width)), 4, *near[0])
        squares, cosine, sine, allowed = lax.optimization_barrier(
            (squares, cosine, sine, allowed)
        )
        weights = (gain, other_gain, own[0], other[0], own[1], other[1])
        kernel = functools.partial(project_kernel, s, sum(STAGES, ()), len(STAGES[-1]))
        outs = (bf16((rows, width)), bf16((ring, columns, rows)))
        query, keyval = call(kernel, outs, 10, squares, *weights, cosine, sine, *sum(near, ()))
        keyval = lax.all_to_all(keyval, Y, 0, 0, tiled=True).reshape(-1, rows)
        attended = call(
            attend_kernel, bf16((FAR_COUNT, rows, width)), 4, query, keyval, cosine, sine, allowed
        )
        near = near_stage(far_stage(attended))
        partial, end = current, s + 1 == sections
        for k, (group, layout) in enumerate(zip(near, STAGES, strict=True)):
            outs, past = (f32((rows, width)),), ()
            if k == stages - 1:
                outs = (bf16((rows, width)),)
                past = (current,) if end else ()
                outs += (bf16((rows, width)),) if end else (bf16((FAR_COUNT, rows, width)),)
            kernel = functools.partial(mix_kernel, s, layout, len(past))
            partial, *extra = call(kernel, outs, 10, own[2], other[2], partial, *past, *group)
        current, copies = partial, extra[0]
    theirs = lax.ppermute(copies, "section", swap)
    return call(place_kernel, bf16((sections, rows, width)), 4, current, theirs)[None]


def solution(mesh):
    finer = Mesh(
        mesh.devices.reshape(mesh.shape["groups"], mesh.shape["section"], *([2] * 6)),
        ("groups", "section") + MESH,
    )
    in_specs = (
        P("groups", None, MESH),
        P("groups", None),
        P("section", None, None),
        P("section", None, None, MESH),
        P("section", None, None, MESH),
        P("section", None, None, MESH),
    )
    out_specs = P("section", "groups", None, MESH)

    return jax.shard_map(
        shards, mesh=finer, in_specs=in_specs, out_specs=out_specs, check_vma=False
    )
```

```python
import functools

import jax
import jax.numpy as jnp
from jax import lax
from jax.experimental import pallas as pl
from jax.experimental.pallas import tpu as pltpu
from jax.sharding import Mesh
from jax.sharding import PartitionSpec as P

HD = 128
HALF = HD // 2
X = ("x2", "x1", "x0")
Y = ("y2", "y1", "y0")
MESH = X + Y
SIDE = 8
FAR_COUNT = 16
norm_epsilon = 1e-05
rope_theta = 500000.0
MIB = 1024 * 1024


def frequencies():
    return rope_theta ** (-(2.0 * jnp.arange(HALF, dtype=jnp.float32)) / HD)


def position_tables(segment_row, freqs):
    row_length = segment_row.shape[0]
    indices = jnp.arange(row_length, dtype=jnp.int32)
    same = segment_row[None, :] == segment_row[:, None]
    first_index = jnp.min(jnp.where(same, indices[None, :], row_length), axis=1)
    positions = (indices - first_index).astype(jnp.float32)
    angles = positions[:, None] * freqs[None, :]
    cosine, sine = jnp.cos(angles), jnp.sin(angles)
    allowed = (indices[None, :] <= indices[:, None]) & same
    return (
        jnp.concatenate([cosine, cosine], axis=1),
        jnp.concatenate([-sine, sine], axis=1),
        allowed.astype(jnp.float32),
    )


STAGES = (((0, 0),), ((1, 0), (3, 0), (2, 0), (2, 2)))
STEP = 4


def colour_groups(sections):
    groups = []
    for section in range(sections):
        one = [[] for _ in range(STEP)]
        for first in range(SIDE):
            for second in range(SIDE):
                x, y = (first, second) if section == 0 else (second, first)
                one[(first + 2 * second) % STEP].append((section * SIDE + x) * SIDE + y)
        groups += one
    return groups


def for_chunks(buffers, layout, body, carry, unrolled=False):
    swapped = lax.axis_index("section") != 0
    x0, x1, y0, y1 = (lax.axis_index(name) for name in ("x0", "x1", "y0", "y1"))
    own_odd = jnp.where(swapped, y0, x0)
    own_half = jnp.where(swapped, y1 + x0, x1 + y0)
    stride, side = jnp.where(swapped, 1, SIDE), jnp.where(swapped, SIDE, 1)
    for ref, (turn, skip) in zip(buffers, layout, strict=True):
        colour = own_odd + 2 * own_half + turn
        odd, half = colour % 2, colour // 2

        def chunk(i, carry, ref=ref, odd=odd, half=half, skip=skip):
            line = i + skip
            place = stride * (odd + 2 * line) + side * ((half + line) % 2)
            return body([(ref[i * STEP + k], place + side * 2 * k) for k in range(STEP)], carry)

        count = ref.shape[0] // STEP
        if unrolled:
            for i in range(count):
                carry = chunk(i, carry)
        else:
            carry = lax.fori_loop(0, count, chunk, carry)
    return carry


def at(place, width):
    return pl.ds(pl.multiple_of(place * width, width), width)


def is_other(section):
    return lax.axis_index("section") != section


def weight_rows(second, own, other, chunk, width):
    parts = []
    for _, place in chunk:
        parts.append(jnp.where(second, other[at(place, width), :], own[at(place, width), :]))
    return jnp.concatenate(parts, axis=0)


def squares_of(buffers, total):
    for ref in buffers:
        for j in range(ref.shape[0]):
            part = ref[j].astype(jnp.float32)
            total += part * part
    return total


def squares_kernel(own_set, total):
    total[...] = squares_of((own_set,), jnp.zeros(total.shape, jnp.float32))


def project_kernel(section, layout, late, squares, *rest):
    gain_own, gain_other, own, other, kv_own, kv_other, cosine, sine = rest[:8]
    buffers, (query, keyval) = rest[8:-2], rest[-2:]
    second = is_other(section)
    rows, width = query.shape
    columns = kv_own.shape[0]
    features = gain_own.shape[1]
    total = squares_of(buffers[-late:], squares[...])
    scale = lax.rsqrt(jnp.sum(total, axis=1, keepdims=True) / features + norm_epsilon)

    def body(chunk, carry):
        q_sum, kv_sum = carry
        normed, kv_parts = [], []
        for part, place in chunk:
            span = at(place, width)
            gain = jnp.where(second, gain_other[:, span], gain_own[:, span]).astype(jnp.float32)
            normed.append((part.astype(jnp.float32) * scale * gain).astype(jnp.bfloat16))
            kv_parts.append(jnp.where(second, kv_other[:, span], kv_own[:, span]))
        normed = jnp.concatenate(normed, axis=1)
        weight = weight_rows(second, own, other, chunk, width)
        q_sum += jnp.dot(normed, weight, preferred_element_type=jnp.float32)
        kv_sum += lax.dot_general(
            normed,
            jnp.concatenate(kv_parts, axis=1),
            (((1,), (1,)), ((), ())),
            preferred_element_type=jnp.float32,
        )
        return q_sum, kv_sum

    zero = jnp.zeros((rows, width), jnp.float32), jnp.zeros((rows, columns), jnp.float32)
    q_sum, kv_sum = for_chunks(buffers, layout, body, zero, unrolled=True)
    turned = jnp.concatenate([q_sum[:, HALF:], q_sum[:, :HALF]], axis=1)
    query[...] = (q_sum * cosine[...] + turned * sine[...]).astype(query.dtype)
    flat = kv_sum.T.astype(keyval.dtype)
    keyval[...] = jnp.broadcast_to(flat[None], keyval.shape)


def attend_kernel(query, keyval, cosine, sine, allowed, attended):
    keys = keyval[:HD, :].astype(jnp.float32)
    turned = jnp.concatenate([keys[HALF:], keys[:HALF]], axis=0)
    keys = (keys * cosine[...].T + turned * sine[...].T).astype(jnp.bfloat16)
    scores = jnp.dot(query[...], keys, preferred_element_type=jnp.float32) * HD ** (-0.5)
    masked = jnp.where(allowed[...] > 0.0, scores, -1e30)
    highest = jnp.max(masked, axis=1, keepdims=True)
    raised = jnp.exp(masked - highest)
    probs = (raised / jnp.sum(raised, axis=1, keepdims=True)).astype(jnp.bfloat16)
    out = lax.dot_general(
        probs, keyval[HD:, :], (((1,), (1,)), ((), ())), preferred_element_type=jnp.float32
    ).astype(jnp.bfloat16)
    attended[...] = jnp.broadcast_to(out[None], attended.shape)


def mix_kernel(section, layout, earlier, own, other, before, *rest):
    past, rest = rest[:earlier], rest[earlier:]
    buffers, outs = rest[: len(layout)], rest[len(layout) :]
    second = is_other(section)
    width = before.shape[1]

    def body(chunk, mixed):
        weight = weight_rows(second, own, other, chunk, width)
        joined = jnp.concatenate([part for part, _ in chunk], axis=1)
        return mixed + jnp.dot(joined, weight, preferred_element_type=jnp.float32)

    mixed = before[...].astype(jnp.float32)
    mixed = for_chunks(buffers, layout, body, mixed, unrolled=len(layout) > 1)
    out = mixed.astype(outs[0].dtype)
    if past:
        lower = lax.axis_index("section") == 0
        outs[0][...] = jnp.where(lower, past[0][...], out)
        outs[1][...] = jnp.where(lower, out, past[0][...])
        return
    outs[0][...] = out
    if len(outs) > 1:
        outs[1][...] = jnp.broadcast_to(out[None], outs[1].shape)


def start_kernel(
    inputs, segments, kv, gains, current, copies, segment_row, kv_out, gains_out, both, sems
):
    me = lax.axis_index("section")
    moves = ((inputs.at[me], current), (segments, both), (kv, kv_out), (gains, gains_out))
    fetches = [pltpu.make_async_copy(a, b, sems.at[k]) for k, (a, b) in enumerate(moves)]
    for fetch in fetches:
        fetch.start()
    fetches[0].wait()
    copies[...] = jnp.broadcast_to(current[...][None], copies.shape)
    fetches[1].wait()
    segment_row[...] = jnp.where(me == 0, both[0:1, :], both[1:2, :])
    fetches[2].wait()
    fetches[3].wait()


def place_kernel(mine, theirs, result):
    me = lax.axis_index("section")
    result[me] = mine[...]
    result[1 - me] = theirs[...]


def call(kernel, outs, limit, *args):
    vmem = pl.BlockSpec(memory_space=pltpu.VMEM)
    return pl.pallas_call(
        kernel,
        out_shape=outs,
        in_specs=[vmem] * len(args),
        out_specs=jax.tree.map(lambda _: vmem, outs),
        compiler_params=pltpu.CompilerParams(vmem_limit_bytes=limit * MIB),
    )(*args)


def from_neighbour(block, first, second):
    pairs = []
    for section in range(lax.axis_size("section")):
        dx, dy = (first, second) if section == 0 else (second, first)
        for x in range(SIDE):
            for y in range(SIDE):
                there = (x + dx) % SIDE * SIDE + (y + dy) % SIDE
                base = section * SIDE * SIDE
                pairs.append((base + there, base + x * SIDE + y))
    return lax.ppermute(block, ("section",) + MESH, pairs)


def far_stage(copies):
    groups = colour_groups(lax.axis_size("section"))
    axes = ("section",) + MESH
    return lax.all_to_all(copies, axes, 0, 0, axis_index_groups=groups, tiled=True)


def near_stage(own):
    half = own.shape[0] // 2
    sets = from_neighbour(own, 1, 0), from_neighbour(own, -1, 0)
    return (own,), sets + (from_neighbour(own[:half], 0, 1), from_neighbour(own[half:], 0, -1))


def shards(inputs, segments, gains, w_query, w_keyval, w_output):
    _, rows, width = inputs.shape
    sections = lax.axis_size("section")
    ring = lax.axis_size(Y)
    swap = [(0, 1), (1, 0)]
    own = [w_query[0, 0], w_keyval[0, 0].T, w_output[0, 0]]
    other = []
    for w in own:
        other.append(lax.ppermute(w, "section", swap))
    other_gain = lax.ppermute(gains[0], "section", swap)
    shape = jax.ShapeDtypeStruct
    bf16 = functools.partial(shape, dtype=jnp.bfloat16)
    f32 = functools.partial(shape, dtype=jnp.float32)
    columns = own[1].shape[0]
    outs = (bf16((rows, width)), bf16((FAR_COUNT, rows, width)), shape((1, rows), jnp.int32))
    outs += (bf16(own[1].shape), bf16(gains[0].shape))
    sources = (inputs, segments, own[1], gains[0])
    anywhere, vmem = pl.BlockSpec(memory_space=pltpu.HBM), pl.BlockSpec(memory_space=pltpu.VMEM)
    current, copies, segment_row, own[1], gain = pl.pallas_call(
        start_kernel,
        out_shape=outs,
        in_specs=[anywhere] * len(sources),
        out_specs=(vmem,) * len(outs),
        scratch_shapes=[
            pltpu.VMEM(segments.shape, segments.dtype),
            pltpu.SemaphoreType.DMA((len(sources),)),
        ],
        compiler_params=pltpu.CompilerParams(vmem_limit_bytes=4 * MIB),
    )(*(pltpu.with_memory_space_constraint(a, pltpu.HBM) for a in sources))
    copies, segment_row, freqs = lax.optimization_barrier((copies, segment_row, frequencies()))
    stages = len(STAGES)
    for s in range(sections):
        far = far_stage(copies)
        if s == 0:
            far, segment_row = lax.optimization_barrier((far, segment_row))
            cosine, sine, allowed = position_tables(segment_row[0], freqs)
        near = near_stage(far)
        squares = call(squares_kernel, f32((rows, width)), 4, *near[0])
        squares, cosine, sine, allowed = lax.optimization_barrier(
            (squares, cosine, sine, allowed)
        )
        weights = (gain, other_gain, own[0], other[0], own[1], other[1])
        kernel = functools.partial(project_kernel, s, sum(STAGES, ()), len(STAGES[-1]))
        outs = (bf16((rows, width)), bf16((ring, columns, rows)))
        query, keyval = call(kernel, outs, 10, squares, *weights, cosine, sine, *sum(near, ()))
        keyval = lax.all_to_all(keyval, Y, 0, 0, tiled=True).reshape(-1, rows)
        attended = call(
            attend_kernel, bf16((FAR_COUNT, rows, width)), 4, query, keyval, cosine, sine, allowed
        )
        near = near_stage(far_stage(attended))
        partial, end = current, s + 1 == sections
        for k, (group, layout) in enumerate(zip(near, STAGES, strict=True)):
            outs, past = (f32((rows, width)),), ()
            if k == stages - 1:
                outs = (bf16((rows, width)),)
                past = (current,) if end else ()
                outs += (bf16((rows, width)),) if end else (bf16((FAR_COUNT, rows, width)),)
            kernel = functools.partial(mix_kernel, s, layout, len(past))
            partial, *extra = call(kernel, outs, 10, own[2], other[2], partial, *past, *group)
        current, copies = partial, extra[0]
    theirs = lax.ppermute(copies, "section", swap)
    return call(place_kernel, bf16((sections, rows, width)), 4, current, theirs)[None]


def solution(mesh):
    finer = Mesh(
        mesh.devices.reshape(mesh.shape["groups"], mesh.shape["section"], *([2] * 6)),
        ("groups", "section") + MESH,
    )
    in_specs = (
        P("groups", None, MESH),
        P("groups", None),
        P("section", None, None),
        P("section", None, None, MESH),
        P("section", None, None, MESH),
        P("section", None, None, MESH),
    )
    out_specs = P("section", "groups", None, MESH)

    return jax.shard_map(
        shards, mesh=finer, in_specs=in_specs, out_specs=out_specs, check_vma=False
    )
```

```python
import functools

import jax
import jax.numpy as jnp
from jax import lax
from jax.experimental import pallas as pl
from jax.experimental.pallas import tpu as pltpu
from jax.sharding import Mesh
from jax.sharding import PartitionSpec as P

HD = 128
HALF = HD // 2
X = ("x2", "x1", "x0")
Y = ("y2", "y1", "y0")
MESH = X + Y
SIDE = 8
FAR_COUNT = 16
norm_epsilon = 1e-05
rope_theta = 500000.0
MIB = 1024 * 1024


def frequencies():
    return rope_theta ** (-(2.0 * jnp.arange(HALF, dtype=jnp.float32)) / HD)


def position_tables(segment_row, freqs):
    row_length = segment_row.shape[0]
    indices = jnp.arange(row_length, dtype=jnp.int32)
    same = segment_row[None, :] == segment_row[:, None]
    first_index = jnp.min(jnp.where(same, indices[None, :], row_length), axis=1)
    positions = (indices - first_index).astype(jnp.float32)
    angles = positions[:, None] * freqs[None, :]
    cosine, sine = jnp.cos(angles), jnp.sin(angles)
    allowed = (indices[None, :] <= indices[:, None]) & same
    return (
        jnp.concatenate([cosine, cosine], axis=1),
        jnp.concatenate([-sine, sine], axis=1),
        allowed.astype(jnp.float32),
    )


STAGES = (((0, 0),), ((1, 0), (3, 0), (2, 0), (2, 2)))
STEP = 4


def member(colour, j):
    step, half = j % SIDE, j // SIDE
    return (colour + 2 * step + 4 * half) % SIDE, step


def colour_groups(sections):
    groups = []
    for section in range(sections):
        for colour in range(STEP):
            group = []
            for j in range(FAR_COUNT):
                first, second = member(colour, j)
                x, y = (first, second) if section == 0 else (second, first)
                group.append((section * SIDE + x) * SIDE + y)
            groups.append(group)
    return groups


def for_chunks(buffers, layout, body, carry):
    swapped = lax.axis_index("section") != 0
    x, y = lax.axis_index(X), lax.axis_index(Y)
    own = jnp.where(swapped, y + 2 * x, x + 2 * y)
    stride, side = jnp.where(swapped, 1, SIDE), jnp.where(swapped, SIDE, 1)
    for ref, (turn, skip) in zip(buffers, layout, strict=True):
        colour = (own + turn) % STEP
        for i in range(0, ref.shape[0], STEP):
            chunk = []
            for j in range(i, i + STEP):
                first, second = member(colour, skip * STEP + j)
                chunk.append((ref[j], stride * first + side * second))
            carry = body(chunk, carry)
    return carry


def at(place, width):
    return pl.ds(pl.multiple_of(place * width, width), width)


def is_other(section):
    return lax.axis_index("section") != section


def weight_rows(second, own, other, chunk, width):
    parts = []
    for _, place in chunk:
        parts.append(jnp.where(second, other[at(place, width), :], own[at(place, width), :]))
    return jnp.concatenate(parts, axis=0)


def squares_of(buffers, total):
    for ref in buffers:
        for j in range(ref.shape[0]):
            part = ref[j].astype(jnp.float32)
            total += part * part
    return total


def squares_kernel(own_set, total):
    total[...] = squares_of((own_set,), jnp.zeros(total.shape, jnp.float32))


def project_kernel(section, layout, late, squares, *rest):
    gain_own, gain_other, own, other, kv_own, kv_other, cosine, sine = rest[:8]
    buffers, (query, keyval) = rest[8:-2], rest[-2:]
    second = is_other(section)
    rows, width = query.shape
    columns = kv_own.shape[0]
    features = gain_own.shape[1]
    total = squares_of(buffers[-late:], squares[...])
    scale = lax.rsqrt(jnp.sum(total, axis=1, keepdims=True) / features + norm_epsilon)

    def body(chunk, carry):
        q_sum, kv_sum = carry
        normed, kv_parts = [], []
        for part, place in chunk:
            span = at(place, width)
            gain = jnp.where(second, gain_other[:, span], gain_own[:, span]).astype(jnp.float32)
            normed.append((part.astype(jnp.float32) * scale * gain).astype(jnp.bfloat16))
            kv_parts.append(jnp.where(second, kv_other[:, span], kv_own[:, span]))
        normed = jnp.concatenate(normed, axis=1)
        weight = weight_rows(second, own, other, chunk, width)
        q_sum += jnp.dot(normed, weight, preferred_element_type=jnp.float32)
        kv_sum += lax.dot_general(
            normed,
            jnp.concatenate(kv_parts, axis=1),
            (((1,), (1,)), ((), ())),
            preferred_element_type=jnp.float32,
        )
        return q_sum, kv_sum

    zero = jnp.zeros((rows, width), jnp.float32), jnp.zeros((rows, columns), jnp.float32)
    q_sum, kv_sum = for_chunks(buffers, layout, body, zero)
    turned = jnp.concatenate([q_sum[:, HALF:], q_sum[:, :HALF]], axis=1)
    query[...] = (q_sum * cosine[...] + turned * sine[...]).astype(query.dtype)
    flat = kv_sum.T.astype(keyval.dtype)
    keyval[...] = jnp.broadcast_to(flat[None], keyval.shape)


def attend_kernel(query, keyval, cosine, sine, allowed, attended):
    keys = keyval[:HD, :].astype(jnp.float32)
    turned = jnp.concatenate([keys[HALF:], keys[:HALF]], axis=0)
    keys = (keys * cosine[...].T + turned * sine[...].T).astype(jnp.bfloat16)
    scores = jnp.dot(query[...], keys, preferred_element_type=jnp.float32) * HD ** (-0.5)
    masked = jnp.where(allowed[...] > 0.0, scores, -1e30)
    highest = jnp.max(masked, axis=1, keepdims=True)
    raised = jnp.exp(masked - highest)
    probs = (raised / jnp.sum(raised, axis=1, keepdims=True)).astype(jnp.bfloat16)
    out = lax.dot_general(
        probs, keyval[HD:, :], (((1,), (1,)), ((), ())), preferred_element_type=jnp.float32
    ).astype(jnp.bfloat16)
    attended[...] = jnp.broadcast_to(out[None], attended.shape)


def mix_kernel(section, layout, earlier, own, other, before, *rest):
    past, rest = rest[:earlier], rest[earlier:]
    buffers, outs = rest[: len(layout)], rest[len(layout) :]
    second = is_other(section)
    width = before.shape[1]

    def body(chunk, mixed):
        weight = weight_rows(second, own, other, chunk, width)
        joined = jnp.concatenate([part for part, _ in chunk], axis=1)
        return mixed + jnp.dot(joined, weight, preferred_element_type=jnp.float32)

    mixed = before[...].astype(jnp.float32)
    mixed = for_chunks(buffers, layout, body, mixed)
    out = mixed.astype(outs[0].dtype)
    if past:
        lower = lax.axis_index("section") == 0
        outs[0][...] = jnp.where(lower, past[0][...], out)
        outs[1][...] = jnp.where(lower, out, past[0][...])
        return
    outs[0][...] = out
    if len(outs) > 1:
        outs[1][...] = jnp.broadcast_to(out[None], outs[1].shape)


def start_kernel(
    inputs, segments, kv, gains, current, copies, segment_row, kv_out, gains_out, both, sems
):
    me = lax.axis_index("section")
    moves = ((inputs.at[me], current), (segments, both), (kv, kv_out), (gains, gains_out))
    fetches = [pltpu.make_async_copy(a, b, sems.at[k]) for k, (a, b) in enumerate(moves)]
    for fetch in fetches:
        fetch.start()
    fetches[0].wait()
    copies[...] = jnp.broadcast_to(current[...][None], copies.shape)
    fetches[1].wait()
    segment_row[...] = jnp.where(me == 0, both[0:1, :], both[1:2, :])
    fetches[2].wait()
    fetches[3].wait()


def place_kernel(mine, theirs, result):
    me = lax.axis_index("section")
    result[me] = mine[...]
    result[1 - me] = theirs[...]


def call(kernel, outs, limit, *args):
    vmem = pl.BlockSpec(memory_space=pltpu.VMEM)
    return pl.pallas_call(
        kernel,
        out_shape=outs,
        in_specs=[vmem] * len(args),
        out_specs=jax.tree.map(lambda _: vmem, outs),
        compiler_params=pltpu.CompilerParams(vmem_limit_bytes=limit * MIB),
    )(*args)


def from_neighbour(block, first, second):
    pairs = []
    for section in range(lax.axis_size("section")):
        dx, dy = (first, second) if section == 0 else (second, first)
        for x in range(SIDE):
            for y in range(SIDE):
                there = (x + dx) % SIDE * SIDE + (y + dy) % SIDE
                base = section * SIDE * SIDE
                pairs.append((base + there, base + x * SIDE + y))
    return lax.ppermute(block, ("section",) + MESH, pairs)


def far_stage(copies):
    groups = colour_groups(lax.axis_size("section"))
    axes = ("section",) + MESH
    return lax.all_to_all(copies, axes, 0, 0, axis_index_groups=groups, tiled=True)


def near_stage(own):
    half = own.shape[0] // 2
    sets = from_neighbour(own, 1, 0), from_neighbour(own, -1, 0)
    return (own,), sets + (from_neighbour(own[:half], 0, 1), from_neighbour(own[half:], 0, -1))


def shards(inputs, segments, gains, w_query, w_keyval, w_output):
    _, rows, width = inputs.shape
    sections = lax.axis_size("section")
    ring = lax.axis_size(Y)
    swap = [(0, 1), (1, 0)]
    own = [w_query[0, 0], w_keyval[0, 0].T, w_output[0, 0]]
    other = []
    for w in own:
        other.append(lax.ppermute(w, "section", swap))
    other_gain = lax.ppermute(gains[0], "section", swap)
    shape = jax.ShapeDtypeStruct
    bf16 = functools.partial(shape, dtype=jnp.bfloat16)
    f32 = functools.partial(shape, dtype=jnp.float32)
    columns = own[1].shape[0]
    outs = (bf16((rows, width)), bf16((FAR_COUNT, rows, width)), shape((1, rows), jnp.int32))
    outs += (bf16(own[1].shape), bf16(gains[0].shape))
    sources = (inputs, segments, own[1], gains[0])
    anywhere, vmem = pl.BlockSpec(memory_space=pltpu.HBM), pl.BlockSpec(memory_space=pltpu.VMEM)
    current, copies, segment_row, own[1], gain = pl.pallas_call(
        start_kernel,
        out_shape=outs,
        in_specs=[anywhere] * len(sources),
        out_specs=(vmem,) * len(outs),
        scratch_shapes=[
            pltpu.VMEM(segments.shape, segments.dtype),
            pltpu.SemaphoreType.DMA((len(sources),)),
        ],
        compiler_params=pltpu.CompilerParams(vmem_limit_bytes=4 * MIB),
    )(*(pltpu.with_memory_space_constraint(a, pltpu.HBM) for a in sources))
    copies, segment_row, freqs = lax.optimization_barrier((copies, segment_row, frequencies()))
    stages = len(STAGES)
    for s in range(sections):
        far = far_stage(copies)
        if s == 0:
            far, segment_row = lax.optimization_barrier((far, segment_row))
            cosine, sine, allowed = position_tables(segment_row[0], freqs)
        near = near_stage(far)
        squares = call(squares_kernel, f32((rows, width)), 4, *near[0])
        squares, cosine, sine, allowed = lax.optimization_barrier(
            (squares, cosine, sine, allowed)
        )
        weights = (gain, other_gain, own[0], other[0], own[1], other[1])
        kernel = functools.partial(project_kernel, s, sum(STAGES, ()), len(STAGES[-1]))
        outs = (bf16((rows, width)), bf16((ring, columns, rows)))
        query, keyval = call(kernel, outs, 10, squares, *weights, cosine, sine, *sum(near, ()))
        keyval = lax.all_to_all(keyval, Y, 0, 0, tiled=True).reshape(-1, rows)
        attended = call(
            attend_kernel, bf16((FAR_COUNT, rows, width)), 4, query, keyval, cosine, sine, allowed
        )
        near = near_stage(far_stage(attended))
        partial, end = current, s + 1 == sections
        for k, (group, layout) in enumerate(zip(near, STAGES, strict=True)):
            outs, past = (f32((rows, width)),), ()
            if k == stages - 1:
                outs = (bf16((rows, width)),)
                past = (current,) if end else ()
                outs += (bf16((rows, width)),) if end else (bf16((FAR_COUNT, rows, width)),)
            kernel = functools.partial(mix_kernel, s, layout, len(past))
            partial, *extra = call(kernel, outs, 10, own[2], other[2], partial, *past, *group)
        current, copies = partial, extra[0]
    theirs = lax.ppermute(copies, "section", swap)
    return call(place_kernel, bf16((sections, rows, width)), 4, current, theirs)[None]


def solution(mesh):
    finer = Mesh(
        mesh.devices.reshape(mesh.shape["groups"], mesh.shape["section"], *([2] * 6)),
        ("groups", "section") + MESH,
    )
    in_specs = (
        P("groups", None, MESH),
        P("groups", None),
        P("section", None, None),
        P("section", None, None, MESH),
        P("section", None, None, MESH),
        P("section", None, None, MESH),
    )
    out_specs = P("section", "groups", None, MESH)

    return jax.shard_map(
        shards, mesh=finer, in_specs=in_specs, out_specs=out_specs, check_vma=False
    )
```

```python
import functools

import jax
import jax.numpy as jnp
from jax import lax
from jax.experimental import pallas as pl
from jax.experimental.pallas import tpu as pltpu
from jax.sharding import Mesh
from jax.sharding import PartitionSpec as P

HD = 128
HALF = HD // 2
X = ("x2", "x1", "x0")
Y = ("y2", "y1", "y0")
MESH = X + Y
SIDE = 8
FAR_COUNT = 16
norm_epsilon = 1e-05
rope_theta = 500000.0
MIB = 1024 * 1024


def position_tables(segment_row, steps):
    row_length = segment_row.shape[0]
    indices = jnp.arange(row_length, dtype=jnp.int32)
    same = segment_row[None, :] == segment_row[:, None]
    first_index = jnp.min(jnp.where(same, indices[None, :], row_length), axis=1)
    positions = (indices - first_index).astype(jnp.float32)
    freqs = rope_theta ** (-(2.0 * steps) / HD)
    angles = positions[:, None] * freqs[None, :]
    cosine, sine = jnp.cos(angles), jnp.sin(angles)
    allowed = (indices[None, :] <= indices[:, None]) & same
    return (
        jnp.concatenate([cosine, cosine], axis=1),
        jnp.concatenate([-sine, sine], axis=1),
        allowed.astype(jnp.float32),
    )


STAGES = (((0, 0),), ((1, 0), (3, 0), (2, 0), (2, 2)))
STEP = 4


def member(colour, j):
    step, half = j % SIDE, j // SIDE
    return (colour + 2 * step + 4 * half) % SIDE, step


def colour_groups(sections):
    groups = []
    for section in range(sections):
        for colour in range(STEP):
            group = []
            for j in range(FAR_COUNT):
                first, second = member(colour, j)
                x, y = (first, second) if section == 0 else (second, first)
                group.append((section * SIDE + x) * SIDE + y)
            groups.append(group)
    return groups


def for_chunks(buffers, layout, body, carry):
    swapped = lax.axis_index("section") != 0
    x, y = lax.axis_index(X), lax.axis_index(Y)
    own = jnp.where(swapped, y + 2 * x, x + 2 * y)
    stride, side = jnp.where(swapped, 1, SIDE), jnp.where(swapped, SIDE, 1)
    for ref, (turn, skip) in zip(buffers, layout, strict=True):
        colour = (own + turn) % STEP
        for i in range(0, ref.shape[0], STEP):
            chunk = []
            for j in range(i, i + STEP):
                first, second = member(colour, skip * STEP + j)
                chunk.append((ref[j], stride * first + side * second))
            carry = body(chunk, carry)
    return carry


def at(place, width):
    return pl.ds(pl.multiple_of(place * width, width), width)


def is_other(section):
    return lax.axis_index("section") != section


def weight_rows(second, own, other, chunk, width):
    parts = []
    for _, place in chunk:
        parts.append(jnp.where(second, other[at(place, width), :], own[at(place, width), :]))
    return jnp.concatenate(parts, axis=0)


def squares_of(buffers, total):
    for ref in buffers:
        for j in range(ref.shape[0]):
            part = ref[j].astype(jnp.float32)
            total += part * part
    return total


def squares_kernel(own_set, total):
    total[...] = squares_of((own_set,), jnp.zeros(total.shape, jnp.float32))


def project_kernel(section, layout, late, squares, *rest):
    gain_own, gain_other, own, other, kv_own, kv_other, cosine, sine = rest[:8]
    buffers, (query, keyval) = rest[8:-2], rest[-2:]
    second = is_other(section)
    rows, width = query.shape
    columns = kv_own.shape[0]
    features = gain_own.shape[1]
    total = squares_of(buffers[-late:], squares[...])
    scale = lax.rsqrt(jnp.sum(total, axis=1, keepdims=True) / features + norm_epsilon)

    def body(chunk, carry):
        q_sum, kv_sum = carry
        normed, kv_parts = [], []
        for part, place in chunk:
            span = at(place, width)
            gain = jnp.where(second, gain_other[:, span], gain_own[:, span]).astype(jnp.float32)
            normed.append((part.astype(jnp.float32) * scale * gain).astype(jnp.bfloat16))
            kv_parts.append(jnp.where(second, kv_other[:, span], kv_own[:, span]))
        normed = jnp.concatenate(normed, axis=1)
        weight = weight_rows(second, own, other, chunk, width)
        q_sum += jnp.dot(normed, weight, preferred_element_type=jnp.float32)
        kv_sum += lax.dot_general(
            normed,
            jnp.concatenate(kv_parts, axis=1),
            (((1,), (1,)), ((), ())),
            preferred_element_type=jnp.float32,
        )
        return q_sum, kv_sum

    zero = jnp.zeros((rows, width), jnp.float32), jnp.zeros((rows, columns), jnp.float32)
    q_sum, kv_sum = for_chunks(buffers, layout, body, zero)
    turned = jnp.concatenate([q_sum[:, HALF:], q_sum[:, :HALF]], axis=1)
    query[...] = (q_sum * cosine[...] + turned * sine[...]).astype(query.dtype)
    flat = kv_sum.T.astype(keyval.dtype)
    keyval[...] = jnp.broadcast_to(flat[None], keyval.shape)


def attend_kernel(query, keyval, cosine, sine, allowed, attended):
    keys = keyval[:HD, :].astype(jnp.float32)
    turned = jnp.concatenate([keys[HALF:], keys[:HALF]], axis=0)
    keys = (keys * cosine[...].T + turned * sine[...].T).astype(jnp.bfloat16)
    scores = jnp.dot(query[...], keys, preferred_element_type=jnp.float32) * HD ** (-0.5)
    masked = jnp.where(allowed[...] > 0.0, scores, -1e30)
    highest = jnp.max(masked, axis=1, keepdims=True)
    raised = jnp.exp(masked - highest)
    probs = (raised / jnp.sum(raised, axis=1, keepdims=True)).astype(jnp.bfloat16)
    out = lax.dot_general(
        probs, keyval[HD:, :], (((1,), (1,)), ((), ())), preferred_element_type=jnp.float32
    ).astype(jnp.bfloat16)
    attended[...] = jnp.broadcast_to(out[None], attended.shape)


def mix_kernel(section, layout, earlier, own, other, before, *rest):
    past, rest = rest[:earlier], rest[earlier:]
    buffers, outs = rest[: len(layout)], rest[len(layout) :]
    second = is_other(section)
    width = before.shape[1]

    def body(chunk, mixed):
        weight = weight_rows(second, own, other, chunk, width)
        joined = jnp.concatenate([part for part, _ in chunk], axis=1)
        return mixed + jnp.dot(joined, weight, preferred_element_type=jnp.float32)

    mixed = before[...].astype(jnp.float32)
    mixed = for_chunks(buffers, layout, body, mixed)
    out = mixed.astype(outs[0].dtype)
    if past:
        lower = lax.axis_index("section") == 0
        outs[0][...] = jnp.where(lower, past[0][...], out)
        outs[1][...] = jnp.where(lower, out, past[0][...])
        return
    outs[0][...] = out
    if len(outs) > 1:
        outs[1][...] = jnp.broadcast_to(out[None], outs[1].shape)


def start_kernel(
    inputs, segments, kv, gains, current, copies, segment_row, kv_out, gains_out, both, sems
):
    me = lax.axis_index("section")
    moves = ((inputs.at[me], current), (segments, both), (kv, kv_out), (gains, gains_out))
    fetches = [pltpu.make_async_copy(a, b, sems.at[k]) for k, (a, b) in enumerate(moves)]
    for fetch in fetches:
        fetch.start()
    fetches[0].wait()
    copies[...] = jnp.broadcast_to(current[...][None], copies.shape)
    fetches[1].wait()
    segment_row[...] = jnp.where(me == 0, both[0:1, :], both[1:2, :])
    fetches[2].wait()
    fetches[3].wait()


def place_kernel(mine, theirs, result):
    me = lax.axis_index("section")
    result[me] = mine[...]
    result[1 - me] = theirs[...]


def call(kernel, outs, limit, *args):
    vmem = pl.BlockSpec(memory_space=pltpu.VMEM)
    return pl.pallas_call(
        kernel,
        out_shape=outs,
        in_specs=[vmem] * len(args),
        out_specs=jax.tree.map(lambda _: vmem, outs),
        compiler_params=pltpu.CompilerParams(vmem_limit_bytes=limit * MIB),
    )(*args)


def from_neighbour(block, first, second):
    pairs = []
    for section in range(lax.axis_size("section")):
        dx, dy = (first, second) if section == 0 else (second, first)
        for x in range(SIDE):
            for y in range(SIDE):
                there = (x + dx) % SIDE * SIDE + (y + dy) % SIDE
                base = section * SIDE * SIDE
                pairs.append((base + there, base + x * SIDE + y))
    return lax.ppermute(block, ("section",) + MESH, pairs)


def far_stage(copies):
    groups = colour_groups(lax.axis_size("section"))
    axes = ("section",) + MESH
    return lax.all_to_all(copies, axes, 0, 0, axis_index_groups=groups, tiled=True)


def near_stage(own):
    half = own.shape[0] // 2
    sets = from_neighbour(own, 1, 0), from_neighbour(own, -1, 0)
    return (own,), sets + (from_neighbour(own[:half], 0, 1), from_neighbour(own[half:], 0, -1))


def shards(inputs, segments, gains, w_query, w_keyval, w_output):
    _, rows, width = inputs.shape
    sections = lax.axis_size("section")
    ring = lax.axis_size(Y)
    swap = [(0, 1), (1, 0)]
    own = [w_query[0, 0], w_keyval[0, 0].T, w_output[0, 0]]
    other = []
    for w in own:
        other.append(lax.ppermute(w, "section", swap))
    other_gain = lax.ppermute(gains[0], "section", swap)
    shape = jax.ShapeDtypeStruct
    bf16 = functools.partial(shape, dtype=jnp.bfloat16)
    f32 = functools.partial(shape, dtype=jnp.float32)
    columns = own[1].shape[0]
    outs = (bf16((rows, width)), bf16((FAR_COUNT, rows, width)), shape((1, rows), jnp.int32))
    outs += (bf16(own[1].shape), bf16(gains[0].shape))
    sources = (inputs, segments, own[1], gains[0])
    anywhere, vmem = pl.BlockSpec(memory_space=pltpu.HBM), pl.BlockSpec(memory_space=pltpu.VMEM)
    current, copies, segment_row, own[1], gain = pl.pallas_call(
        start_kernel,
        out_shape=outs,
        in_specs=[anywhere] * len(sources),
        out_specs=(vmem,) * len(outs),
        scratch_shapes=[
            pltpu.VMEM(segments.shape, segments.dtype),
            pltpu.SemaphoreType.DMA((len(sources),)),
        ],
        compiler_params=pltpu.CompilerParams(vmem_limit_bytes=4 * MIB),
    )(*(pltpu.with_memory_space_constraint(a, pltpu.HBM) for a in sources))
    stages = len(STAGES)
    for s in range(sections):
        far = far_stage(copies)
        near = near_stage(far)
        squares = call(squares_kernel, f32((rows, width)), 4, *near[0])
        if s == 0:
            steps = jnp.arange(HALF, dtype=jnp.float32)
            squares, segment_row, steps = lax.optimization_barrier((squares, segment_row, steps))
            cosine, sine, allowed = position_tables(segment_row[0], steps)
        squares, cosine, sine, allowed = lax.optimization_barrier(
            (squares, cosine, sine, allowed)
        )
        weights = (gain, other_gain, own[0], other[0], own[1], other[1])
        kernel = functools.partial(project_kernel, s, sum(STAGES, ()), len(STAGES[-1]))
        outs = (bf16((rows, width)), bf16((ring, columns, rows)))
        query, keyval = call(kernel, outs, 10, squares, *weights, cosine, sine, *sum(near, ()))
        keyval = lax.all_to_all(keyval, Y, 0, 0, tiled=True).reshape(-1, rows)
        attended = call(
            attend_kernel, bf16((FAR_COUNT, rows, width)), 4, query, keyval, cosine, sine, allowed
        )
        near = near_stage(far_stage(attended))
        partial, end = current, s + 1 == sections
        for k, (group, layout) in enumerate(zip(near, STAGES, strict=True)):
            outs, past = (f32((rows, width)),), ()
            if k == stages - 1:
                outs = (bf16((rows, width)),)
                past = (current,) if end else ()
                outs += (bf16((rows, width)),) if end else (bf16((FAR_COUNT, rows, width)),)
            kernel = functools.partial(mix_kernel, s, layout, len(past))
            partial, *extra = call(kernel, outs, 10, own[2], other[2], partial, *past, *group)
        current, copies = partial, extra[0]
    theirs = lax.ppermute(copies, "section", swap)
    return call(place_kernel, bf16((sections, rows, width)), 4, current, theirs)[None]


def solution(mesh):
    finer = Mesh(
        mesh.devices.reshape(mesh.shape["groups"], mesh.shape["section"], *([2] * 6)),
        ("groups", "section") + MESH,
    )
    in_specs = (
        P("groups", None, MESH),
        P("groups", None),
        P("section", None, None),
        P("section", None, None, MESH),
        P("section", None, None, MESH),
        P("section", None, None, MESH),
    )
    out_specs = P("section", "groups", None, MESH)

    return jax.shard_map(
        shards, mesh=finer, in_specs=in_specs, out_specs=out_specs, check_vma=False
    )
```
